8 devices in a mesh: rep: 1 (over z), r: 2 (over y), s: 4 (over x, core).
Axes of the slice: x: 2, y: 2, z: 1, core: 2. Of those that a mesh axis runs over, the one named last changes fastest.
Arguments:
- x: bfloat16 [8, 4096, 768], P(('rep', 'r', 's'))
- dy: bfloat16 [8, 4096, 768], P(('rep', 'r', 's'))
- w_gate: bfloat16 [2, 768, 6144], P(None, 's')
- w_up: bfloat16 [2, 768, 6144], P(None, 's')
- w_down: bfloat16 [2, 6144, 768], P(None, 's')
Outputs:
- output 1: bfloat16 [8, 4096, 768], P(('rep', 'r', 's'))
- output 2: bfloat16 [2, 768, 6144], P('rep', 's')
- output 3: bfloat16 [2, 768, 6144], P('rep', 's')
- output 4: bfloat16 [2, 6144, 768], P('rep', 's')
All inputs are finite; a program needn't handle non-finite values.
Results may differ from the reference program's by a relative error of at most 0.018.
Values are sent between devices in bfloat16 or wider.
A program may use at most 2 GiB of HBM per device.

```python
import jax
import jax.numpy as jnp
from jax import lax

SEQUENCES = 8
TOKENS = 4096
D = 768
FF = 6144
LAYERS = 2
NAMES = ("w_gate", "w_up", "w_down")
SHAPES = {"w_gate": (LAYERS, D, FF), "w_up": (LAYERS, D, FF), "w_down": (LAYERS, FF, D)}


def bump(key, n, height):
    away = (jnp.arange(n, dtype=jnp.int32) - jax.random.randint(key, (), 0, n, jnp.int32)) % n
    return jnp.where(away < n // 8, height, 1.0)


def together(key, own, strength):
    shared = jax.random.normal(key, own.shape[1:], jnp.float32)
    return (own + strength * shared) * lax.rsqrt(1 + strength * strength)


def setup_inputs(seed: int = 0, part: int = 0) -> dict:
    kx, kdy, ka, kb, kz, kf, kh, kl, *kw = jax.random.split(jax.random.key(seed), 8 + len(NAMES))
    kx, kdy, ka, kb = (jax.random.fold_in(k, part) for k in (kx, kdy, ka, kb))
    shape = (SEQUENCES, TOKENS, D)
    much_x, much_dy = jax.random.uniform(kz, (2,), jnp.float32, 0.0, 1.0)
    layers = 2.0 ** jax.random.uniform(kl, (LAYERS, 1, 1), jnp.float32, -1.0, 1.0)
    x = together(ka, jax.random.normal(kx, shape, jnp.float32), much_x) * bump(kf, D, 4.0)
    dy = together(kb, jax.random.normal(kdy, shape, jnp.float32), much_dy)
    drawn = {"x": x.astype(jnp.bfloat16), "dy": (dy * (SEQUENCES * TOKENS) ** -0.5).astype(jnp.bfloat16)}
    for key, name in zip(kw, NAMES, strict=True):
        w = jax.random.normal(key, SHAPES[name], jnp.float32) * SHAPES[name][1] ** -0.5
        drawn[name] = (w * {"w_gate": 1.0, "w_up": bump(kh, FF, 4.0), "w_down": layers}[name]).astype(jnp.bfloat16)
    return drawn


def matmul(a, w):
    return jnp.dot(a, w, preferred_element_type=jnp.float32).astype(jnp.bfloat16)


def normed(h):
    wide = h.astype(jnp.float32)
    scale = lax.rsqrt(jnp.mean(wide**2, -1, keepdims=True) + 1e-6)
    return (wide * scale).astype(jnp.bfloat16)


def layer(h, w):
    a = normed(h)
    gate = jnp.dot(a, w["w_gate"], preferred_element_type=jnp.float32)
    up = jnp.dot(a, w["w_up"], preferred_element_type=jnp.float32)
    return h + matmul((jax.nn.silu(gate) * up).astype(jnp.bfloat16), w["w_down"])


def stack(weights, h):
    return lax.scan(lambda h, w: (layer(h, w), None), h, weights)[0]


def reference(x, dy, w_gate, w_up, w_down):
    weights = dict(zip(NAMES, (w_gate, w_up, w_down), strict=True))

    def take(so_far, sequence):
        h, by_y = sequence
        _, back = jax.vjp(stack, weights, h)
        by_weights, by_h = back(by_y)
        return jax.tree.map(lambda total, term: total + term.astype(jnp.float32), so_far, by_weights), by_h

    none_yet = {name: jnp.zeros(w.shape, jnp.float32) for name, w in weights.items()}
    by_weights, by_x = lax.scan(take, none_yet, (x, dy))
    return (by_x, *(by_weights[name].astype(jnp.bfloat16) for name in NAMES))
```

```python
import functools

import jax
import jax.numpy as jnp
from jax import lax
from jax.experimental import pallas as pl
from jax.experimental.pallas import tpu as pltpu
from jax.sharding import PartitionSpec as P

f32, bf16 = jnp.float32, jnp.bfloat16
TOK, D, FF, L = 4096, 768, 6144, 2
S = 4
C = 512
J = FF // C
W = C // S
RD, RF = D // S, FF // S
PR = 2 * RD + W * D // C
VM = 67043328
once = pl.Buffered(1)


def dot(a, b, ca=1, cb=0):
    return lax.dot_general(a, b, (((ca,), (cb,)), ((), ())), preferred_element_type=f32)


def normed(wide):
    scale = lax.rsqrt(jnp.mean(wide**2, -1, keepdims=True) + 1e-6)
    return wide * scale, scale


def gate_of(w):
    return jnp.concatenate([w[s, 0:RD, :] for s in range(S)], axis=0)


def up_of(w):
    return jnp.concatenate([w[s, RD : 2 * RD, :] for s in range(S)], axis=0)


def down_of(w, at=2 * RD):
    def rows(s):
        fold = jnp.concatenate([w[s, at + W : at + W + W // 2, 0 : D - C], w[s, at + W : at + W + W // 2, D - C : 2 * (D - C)]], axis=0)
        return jnp.concatenate([w[s, at : at + W, :], fold], axis=1)

    return jnp.concatenate([rows(s) for s in range(S)], axis=0)


def piece_slices(j):
    for s in range(S):
        cols = pl.ds(pl.multiple_of(RF * s + W * j, W), W)
        yield 0, (pl.ds(0, RD), cols), (pl.ds(0, RD), pl.ds(W * s, W))
        yield 1, (pl.ds(0, RD), cols), (pl.ds(RD, RD), pl.ds(W * s, W))
    at = pl.multiple_of(W * j, W)
    yield 2, (pl.ds(at, W), pl.ds(0, C)), (pl.ds(2 * RD, W), pl.ds(0, C))
    yield 2, (pl.ds(at, W // 2), pl.ds(C, D - C)), (pl.ds(2 * RD + W, W // 2), pl.ds(0, D - C))
    yield 2, (pl.ds(at + W // 2, W // 2), pl.ds(C, D - C)), (pl.ds(2 * RD + W, W // 2), pl.ds(D - C, D - C))


def prep_kernel(x, wg, wu, wd, a, at, whole, stage, sems):
    i = pl.program_id(0)
    me = lax.axis_index("s")
    n = pl.num_programs(0)
    per = L * J // 8
    slot = lax.rem(i, 2)
    for q in range(per):
        k = i * per + q
        l, j = k // J, lax.rem(k, J)
        for m, src, dst in piece_slices(j):
            pltpu.make_async_copy((wg, wu, wd)[m].at[(l, *src)], stage.at[(slot, q, *dst)], sems.at[0, q]).start()
    y, _ = normed(x[...].astype(f32))
    y = y.astype(bf16)
    a[...] = y
    at[...] = y.T
    for q in range(per):
        k = i * per + q
        l, j = k // J, lax.rem(k, J)
        pltpu.make_async_copy(whole.at[l, me, j], stage.at[slot, q], sems.at[0, q]).wait()

        @pl.when(i > 0)
        def _():
            pltpu.make_async_copy(stage.at[1 - slot, q], whole.at[l, me, j], sems.at[1, q]).wait()

        out = pltpu.make_async_copy(stage.at[slot, q], whole.at[l, me, j], sems.at[1, q])
        out.start()

        @pl.when(i == n - 1)
        def _():
            out.wait()


def prep(x, wg, wu, wd):
    T = TOK // 8
    hbm = pl.BlockSpec(memory_space=pl.ANY)
    return pl.pallas_call(
        prep_kernel,
        grid=(8,),
        in_specs=[pl.BlockSpec((T, D), lambda i: (i, 0)), hbm, hbm, hbm],
        out_specs=[pl.BlockSpec((T, D), lambda i: (i, 0)), pl.BlockSpec((D, T), lambda i: (0, i)), hbm],
        out_shape=[jax.ShapeDtypeStruct((TOK, D), bf16), jax.ShapeDtypeStruct((D, TOK), bf16), jax.ShapeDtypeStruct((L, S, J, PR, C), bf16)],
        scratch_shapes=[pltpu.VMEM((2, L * J // 8, PR, C), bf16), pltpu.SemaphoreType.DMA((2, L * J // 8))],
        compiler_params=pltpu.CompilerParams(vmem_limit_bytes=VM),
        name="prep",
    )(x, wg, wu, wd)


MESH = pl.DeviceIdType.MESH
HALF = PR // 2
hbm = pl.BlockSpec(memory_space=pl.ANY)


def place():
    me, y = lax.axis_index("s"), lax.axis_index("r")
    return me, y, {"s": me + 1 - 2 * lax.rem(me, 2)}, {"s": lax.rem(me + 2, S)}, {"r": 1 - y}


def greet():
    _, _, core, across, copy = place()
    barrier = pltpu.get_barrier_semaphore()
    for to in (core, across, copy):
        pl.semaphore_signal(barrier, inc=1, device_id=to, device_id_type=MESH)
    pl.semaphore_wait(barrier, 3)


def remote(src, dst, send, recv, to):
    return pltpu.make_async_remote_copy(src_ref=src, dst_ref=dst, send_sem=send, recv_sem=recv, device_id=to, device_id_type=MESH)


class Gather:
    def __init__(self, whole, send, recv, first):
        self.whole, self.send, self.recv, self.first = whole, send, recv, first

    def copy(self, k, n):
        me, y, core, across, copy = place()
        l, j = k // J, lax.rem(k, J)
        near, far = pl.ds(pl.multiple_of(HALF * y, HALF), HALF), pl.ds(pl.multiple_of(HALF * (1 - y), HALF), HALF)
        s = me if n < 2 else lax.rem(me + 2, S)
        what = self.whole.at[(l, s, j, *((), (near,), (near,), (near,), (far,))[n])]
        return remote(what, what, self.send.at[lax.rem(k, 8), n], self.recv.at[k - self.first, n], (core, across, copy, core, core)[n])

    def start(self, k):
        self.copy(k, 0).start()
        self.copy(k, 1).start()

    def across(self, k):
        self.copy(k, 1).wait_recv()
        self.copy(k, 2).start()
        self.copy(k, 3).start()

    def along(self, k):
        self.copy(k, 2).wait_recv()
        self.copy(k, 4).start()

    def finish(self, k):
        for n in (0, 3, 4):
            self.copy(k, n).wait_recv()
        for n in range(5):
            self.copy(k, n).wait_send()


def fetch(whole, held, sem, l, j):
    slot = lax.rem(j, 2)
    return [pltpu.make_async_copy(whole.at[l, s, j], held.at[slot, s], sem.at[slot, s]) for s in range(S)]


AHEAD = 5
EARLY = 2


def forward_kernel(a, x, _, h, a1, a1t, gs, us, whole, acc, held, send, recv, load):
    j, t = pl.program_id(0), pl.program_id(1)
    T = h.shape[0]
    gather = Gather(whole, send, recv, 0)
    K = J + EARLY

    @pl.when((j == 0) & (t == 0))
    def _():
        greet()
        for k in range(AHEAD):
            gather.start(k)
        gather.across(0)
        gather.across(1)
        gather.along(0)
        gather.finish(0)
        for copy in fetch(whole, held, load, 0, 0):
            copy.start()

    @pl.when(t == 0)
    def _():
        for copy in fetch(whole, held, load, 0, j):
            copy.wait()

        @pl.when(j + AHEAD < K)
        def _():
            gather.start(j + AHEAD)

    @pl.when((t == 1) & (j + 2 < K))
    def _():
        gather.across(j + 2)

    @pl.when(t == 2)
    def _():
        gather.along(j + 1)

    @pl.when(t == 3)
    def _():
        gather.finish(j + 1)

        @pl.when(j + 1 < J)
        def _():
            for copy in fetch(whole, held, load, 0, j + 1):
                copy.start()

    rows = pl.ds(pl.multiple_of(t * T, T), T)
    w = held.at[lax.rem(j, 2)]
    lhs = a[rows, :]
    g, u = dot(lhs, gate_of(w)), dot(lhs, up_of(w))
    gs[0], us[0] = g, u
    act = (g * jax.nn.sigmoid(g) * u).astype(bf16)
    acc[rows, :] = jnp.where(j == 0, 0.0, acc[rows, :]) + dot(act, down_of(w))

    @pl.when(j == J - 1)
    def _():
        out = x[...].astype(f32) + acc[rows, :].astype(bf16).astype(f32)
        out = out.astype(bf16)
        h[...] = out
        y, _ = normed(out.astype(f32))
        y = y.astype(bf16)
        a1[...] = y
        a1t[...] = y.T

    @pl.when((j == J - 1) & (t == pl.num_programs(1) - 1))
    def _():
        gather.along(J + 1)
        gather.finish(J + 1)


def forward(a, x, whole):
    T = 1024
    last = lambda j, t: (jnp.where(j == J - 1, t, 0), 0)
    lastT = lambda j, t: (0, jnp.where(j == J - 1, t, 0))
    return pl.pallas_call(
        forward_kernel,
        grid=(J, TOK // T),
        in_specs=[pl.BlockSpec((TOK, D), lambda j, t: (0, 0), pipeline_mode=once), pl.BlockSpec((T, D), last), hbm],
        out_specs=[pl.BlockSpec((T, D), last)] * 2 + [pl.BlockSpec((D, T), lastT)] + [pl.BlockSpec((1, T, C), lambda j, t: (j, t, 0))] * 2 + [hbm],
        out_shape=[jax.ShapeDtypeStruct((TOK, D), bf16)] * 2
        + [jax.ShapeDtypeStruct((D, TOK), bf16)]
        + [jax.ShapeDtypeStruct((J, TOK, C), f32)] * 2
        + [jax.ShapeDtypeStruct((L, S, J, PR, C), bf16)],
        scratch_shapes=[
            pltpu.VMEM((TOK, D), f32),
            pltpu.VMEM((2, S, PR, C), bf16),
            pltpu.SemaphoreType.DMA((8, 5)),
            pltpu.SemaphoreType.DMA((J + EARLY, 5)),
            pltpu.SemaphoreType.DMA((2, S)),
        ],
        input_output_aliases={2: 5},
        compiler_params=pltpu.CompilerParams(vmem_limit_bytes=VM, collective_id=0, has_side_effects=True),
        cost_estimate=pl.CostEstimate(flops=6 * TOK * D * FF, bytes_accessed=250 << 20, transcendentals=0),
        name="forward",
    )(a, x, whole)


def pack(s, ag, au, ad):
    rows = pl.ds(pl.multiple_of(RD * s, RD), RD)
    down = ad[:, pl.ds(pl.multiple_of(W * s, W), W)].T
    yield slice(0, RD), slice(0, C), ag[rows, :]
    yield slice(RD, 2 * RD), slice(0, C), au[rows, :]
    yield slice(2 * RD, 2 * RD + W), slice(0, C), down[:, :C]
    yield slice(2 * RD + W, PR), slice(0, D - C), down[: W // 2, C:]
    yield slice(2 * RD + W, PR), slice(D - C, C), down[W // 2 :, C:]


class Reduce:
    def __init__(self, sums, theirs, kept, out_a, in_a, kept_b, out_b, in_b, out_c, sa, sb, sc):
        self.sums, self.theirs = sums, theirs
        self.kept, self.out_a, self.in_a = kept, out_a, in_a
        self.kept_b, self.out_b, self.in_b, self.out_c = kept_b, out_b, in_b, out_c
        self.sa, self.sb, self.sc = sa, sb, sc

    def copy_a(self, j):
        slot = lax.rem(j, 2)
        return remote(self.out_a, self.in_a.at[slot], self.sa.at[0, 0], self.sa.at[1, slot], place()[2])

    def copy_b(self, j):
        slot = lax.rem(j, 2)
        return remote(self.out_b, self.in_b.at[slot], self.sb.at[0, 0], self.sb.at[1, slot], place()[3])

    def copy_c(self, j):
        slot = lax.rem(j, 2)
        return remote(self.out_c, self.theirs.at[j], self.sc.at[0, 0], self.sc.at[1, slot], place()[4])

    def store_c(self, j):
        return pltpu.make_async_copy(self.out_c, self.sums.at[j], self.sc.at[0, 1])

    def collect(self, ag, au, ad):
        c = lax.rem(lax.axis_index("s"), 2)
        for x in range(2):
            for r, cols, v in pack(2 * x + c, ag, au, ad):
                self.kept[x, r, cols] = v
            for r, cols, v in pack(2 * x + 1 - c, ag, au, ad):
                self.out_a[x, r, cols] = v.astype(bf16)

    def add_a(self, j):
        slot = lax.rem(j, 2)
        x = lax.axis_index("s") // 2
        self.kept_b[...] = self.kept[x] + self.in_a[slot, x].astype(f32)
        self.out_b[...] = (self.kept[1 - x] + self.in_a[slot, 1 - x].astype(f32)).astype(bf16)

    def add_b(self, j):
        self.out_c[...] = (self.kept_b[...] + self.in_b[lax.rem(j, 2)].astype(f32)).astype(bf16)


REDUCE_SCRATCH = [
    pltpu.VMEM((2, PR, C), f32),
    pltpu.VMEM((2, PR, C), bf16),
    pltpu.VMEM((2, 2, PR, C), bf16),
    pltpu.VMEM((PR, C), f32),
    pltpu.VMEM((PR, C), bf16),
    pltpu.VMEM((2, PR, C), bf16),
    pltpu.VMEM((PR, C), bf16),
    pltpu.SemaphoreType.DMA((2, 2)),
    pltpu.SemaphoreType.DMA((2, 2)),
    pltpu.SemaphoreType.DMA((2, 2)),
]


def weights_kernel(saved, *refs):
    if saved:
        at, dy, dyt, w, gs, us, sums, theirs, kept_o, out_o, dgs, dus, ag, au, ad, save, *rest = refs
    else:
        a, at, dy, dyt, _, sums, theirs, kept_o, out_o, dgs, dus, whole, ag, au, ad, save, held, send, recv, load, *rest = refs
        gather = Gather(whole, send, recv, J)
    reduce = Reduce(sums, theirs, *rest)
    j, t = pl.program_id(0), pl.program_id(1)
    T = dgs.shape[1]

    @pl.when((j == 0) & (t == 0))
    def _():
        greet()
        if not saved:
            gather.start(J + EARLY)
            for copy in fetch(whole, held, load, 1, 0):
                copy.start()

    if not saved:

        @pl.when(t == 0)
        def _():
            for copy in fetch(whole, held, load, 1, j):
                copy.wait()

            @pl.when(j + EARLY + 1 < J)
            def _():
                gather.start(J + j + EARLY + 1)

        @pl.when((t == 2) & (j + 2 >= EARLY) & (j + 2 < J))
        def _():
            gather.across(J + j + 2)

        @pl.when((t == 1) & (j + 1 >= EARLY) & (j + 1 < J))
        def _():
            gather.along(J + j + 1)

        @pl.when((t == 3) & (j + 1 < J))
        def _():
            @pl.when(j + 1 >= EARLY)
            def _():
                gather.finish(J + j + 1)

            for copy in fetch(whole, held, load, 1, j + 1):
                copy.start()

    @pl.when(t == 1)
    def _():
        @pl.when(j >= 3)
        def _():
            reduce.copy_c(j - 3).wait()
            reduce.store_c(j - 3).wait()

        @pl.when(j >= 2)
        def _():
            reduce.copy_b(j - 2).wait()
            reduce.add_b(j - 2)
            reduce.copy_c(j - 2).start()
            reduce.store_c(j - 2).start()

        @pl.when(j >= 1)
        def _():
            reduce.copy_a(j - 1).wait()
            reduce.add_a(j - 1)
            reduce.copy_b(j - 1).start()

    rows = pl.ds(pl.multiple_of(t * T, T), T)
    if saved:
        g, u = gs[0], us[0]
        down = down_of(w.at[0, :, 0], 0)
    else:
        w = held.at[lax.rem(j, 2)]
        lhs = a[rows, :]
        g, u = dot(lhs, gate_of(w)), dot(lhs, up_of(w))
        down = down_of(w)
    by = dot(dy[rows, :], down, 1, 1).astype(bf16).astype(f32)
    sig = jax.nn.sigmoid(g)
    silu = g * sig
    act = (silu * u).astype(bf16)
    du = (by * silu).astype(bf16)
    dg = (by * u * (sig + silu * (1 - sig))).astype(bf16)
    dgs[0], dus[0] = dg, du
    for acc, l, r in ((ag, at, dg), (au, at, du), (ad, dyt, act)):
        acc[...] = jnp.where(t == 0, 0.0, acc[...]) + dot(l[:, rows], r)

    @pl.when(t == pl.num_programs(1) - 1)
    def _():
        reduce.collect(ag, au, ad)

        @pl.when(j < J - 1)
        def _():
            reduce.copy_a(j).start()

        @pl.when(j == J - 1)
        def _():
            handed = [pltpu.make_async_copy(reduce.kept, kept_o, save.at[0]), pltpu.make_async_copy(reduce.out_a, out_o, save.at[1])]
            for copy in handed:
                copy.start()
            reduce.copy_c(J - 3).wait()
            reduce.store_c(J - 3).wait()
            reduce.copy_b(J - 2).wait()
            reduce.add_b(J - 2)
            reduce.store_c(J - 2).start()
            reduce.store_c(J - 2).wait()
            for copy in handed:
                copy.wait()


def weights_pass(saved, a, at, dy, dyt, whole, gs=None, us=None):
    T = 1024
    full = lambda shape: pl.BlockSpec(shape, lambda j, t: (0, 0), pipeline_mode=once)
    tile = pl.BlockSpec((1, T, C), lambda j, t: (j, t, 0))
    outs = [hbm] * 4 + [tile, tile]
    shapes = [
        jax.ShapeDtypeStruct((J, PR, C), bf16),
        jax.ShapeDtypeStruct((J, PR, C), bf16),
        jax.ShapeDtypeStruct((2, PR, C), f32),
        jax.ShapeDtypeStruct((2, PR, C), bf16),
    ] + [jax.ShapeDtypeStruct((J, TOK, C), bf16)] * 2
    scratch = [pltpu.VMEM((D, C), f32)] * 3 + [pltpu.SemaphoreType.DMA((2,))]
    if saved:
        ins = [full((D, TOK)), full((TOK, D)), full((D, TOK)), pl.BlockSpec((1, S, 1, PR - 2 * RD, C), lambda j, t: (0, 0, j, 2, 0)), tile, tile]
        args = (at, dy, dyt, whole, gs, us)
        alias = {}
    else:
        ins = [full((TOK, D)), full((D, TOK)), full((TOK, D)), full((D, TOK)), hbm]
        args = (a, at, dy, dyt, whole)
        outs.append(hbm)
        shapes.append(jax.ShapeDtypeStruct((L, S, J, PR, C), bf16))
        alias = {4: 6}
        scratch += [
            pltpu.VMEM((2, S, PR, C), bf16),
            pltpu.SemaphoreType.DMA((8, 5)),
            pltpu.SemaphoreType.DMA((J, 5)),
            pltpu.SemaphoreType.DMA((2, S)),
        ]
    return pl.pallas_call(
        functools.partial(weights_kernel, saved),
        grid=(J, TOK // T),
        in_specs=ins,
        out_specs=outs,
        out_shape=shapes,
        scratch_shapes=scratch + REDUCE_SCRATCH,
        input_output_aliases=alias,
        compiler_params=pltpu.CompilerParams(vmem_limit_bytes=VM, collective_id=2 if saved else 1, has_side_effects=True),
        cost_estimate=pl.CostEstimate(flops=(8 if saved else 12) * TOK * D * FF, bytes_accessed=300 << 20, transcendentals=0),
        name="weights_saved" if saved else "weights_again",
    )(*args)


def norm_back(by, h, dy):
    wide = h.astype(f32)
    scale = lax.rsqrt(jnp.mean(wide**2, -1, keepdims=True) + 1e-6)
    dot_ = jnp.sum(by * wide, -1, keepdims=True) / D
    by_h = (by * scale - wide * (scale * scale * scale * dot_)).astype(bf16)
    return (dy.astype(f32) + by_h.astype(f32)).astype(bf16)


Q = 2


def contract(j, dgs, dus, w, acc):
    total = jnp.where(j == 0, 0.0, acc[...])
    for q in range(Q):
        total = total + dot(dgs[q], gate_of(w.at[0, :, q]), 1, 1)
        total = total + dot(dus[q], up_of(w.at[0, :, q]), 1, 1)
    acc[...] = total


def input_kernel(transpose, dgs, dus, w, h, dy, sums_i, theirs_i, kept_i, out_i, *refs):
    if transpose:
        out, outt, sums, theirs, acc, load, *rest = refs
    else:
        out, sums, theirs, acc, load, *rest = refs
    reduce = Reduce(sums, theirs, *rest)
    t, j = pl.program_id(0), pl.program_id(1)
    step = t * pl.num_programs(1) + j
    second = lambda: remote(sums.at[J - 2], theirs.at[J - 2], load.at[1], load.at[2], place()[4])
    first = lambda: remote(out_i, reduce.in_a.at[1], reduce.sa.at[0, 0], reduce.sa.at[1, 1], place()[2])
    kept = lambda: pltpu.make_async_copy(kept_i, reduce.kept, load.at[0])

    @pl.when(step == 0)
    def _():
        greet()
        first().start()
        second().start()
        kept().start()

    @pl.when(step == 1)
    def _():
        first().wait()
        kept().wait()
        reduce.add_a(J - 1)
        reduce.copy_b(J - 1).start()

    @pl.when(step == 6)
    def _():
        reduce.copy_b(J - 1).wait()
        reduce.add_b(J - 1)
        reduce.copy_c(J - 1).start()
        reduce.store_c(J - 1).start()

    @pl.when(step == 11)
    def _():
        second().wait()
        reduce.copy_c(J - 1).wait()
        reduce.store_c(J - 1).wait()

    contract(j, dgs, dus, w, acc)

    @pl.when(j == pl.num_programs(1) - 1)
    def _():
        by = norm_back(acc[...].astype(bf16).astype(f32), h[...], dy[...])
        out[...] = by
        if transpose:
            outt[...] = by.T


def input_pass(l, dgs, dus, whole, h, dy, sums, theirs, kept, out_a):
    T = 1024
    n = TOK if l else TOK // 2
    tile = pl.BlockSpec((Q, T, C), lambda t, j: (j, t, 0))
    row = pl.BlockSpec((T, D), lambda t, j: (t, 0))
    return pl.pallas_call(
        functools.partial(input_kernel, l == 1),
        grid=(n // T, J // Q),
        in_specs=[tile, tile, pl.BlockSpec((1, S, Q, 2 * RD, C), lambda t, j: (l, 0, j, 0, 0)), row, row] + [hbm] * 4,
        out_specs=([row, pl.BlockSpec((D, T), lambda t, j: (0, t))] if l else [row]) + [hbm] * 2,
        out_shape=([jax.ShapeDtypeStruct((TOK, D), bf16), jax.ShapeDtypeStruct((D, TOK), bf16)] if l else [jax.ShapeDtypeStruct((n, D), bf16)])
        + [jax.ShapeDtypeStruct((J, PR, C), bf16)] * 2,
        scratch_shapes=[pltpu.VMEM((T, D), f32), pltpu.SemaphoreType.DMA((3,))] + REDUCE_SCRATCH,
        input_output_aliases={5: 2, 6: 3} if l else {5: 1, 6: 2},
        compiler_params=pltpu.CompilerParams(vmem_limit_bytes=VM, collective_id=3 + l, has_side_effects=True),
        cost_estimate=pl.CostEstimate(flops=4 * n * D * FF, bytes_accessed=150 << 20, transcendentals=0),
        name="input_pass",
    )(dgs, dus, whole, h, dy, sums, theirs, kept, out_a)


def last_kernel(dgs, dus, w, h, dy, begun, s1, t1, s0, t0, out, og, ou, od, acc, stage, sems):
    t, j = pl.program_id(0), pl.program_id(1)
    i = t * pl.num_programs(1) + j
    slot = lax.rem(i, 2)

    def copies(l):
        for m, dst, src in piece_slices(i):
            yield pltpu.make_async_copy(stage.at[(slot, l, *src)], (og, ou, od)[m].at[(l, *dst)], sems.at[slot, l])

    def wait(slot):
        for l in range(L):
            pltpu.make_async_copy(stage.at[slot, l], stage.at[slot, l], sems.at[slot, l]).wait()

    @pl.when(i >= 2)
    def _():
        wait(slot)

    for l, (mine, other) in enumerate(((s0, t0), (s1, t1))):
        stage[slot, l] = (mine[0].astype(f32) + other[0].astype(f32)).astype(bf16)
    contract(j, dgs, dus, w, acc)
    for l in range(L):
        for copy in copies(l):
            copy.start()

    @pl.when(j == pl.num_programs(1) - 1)
    def _():
        out[0] = begun[...]
        out[1] = norm_back(acc[...].astype(bf16).astype(f32), h[...], dy[...])

    @pl.when(i == J - 1)
    def _():
        wait(slot)
        wait(1 - slot)


def last_pass(dgs, dus, whole, h, dy, begun, s1, t1, s0, t0):
    T = 1024
    n = TOK // 2 // T
    steps = J // Q
    assert n * steps == J
    tile = pl.BlockSpec((Q, T, C), lambda t, j: (j, t + n, 0))
    row = pl.BlockSpec((T, D), lambda t, j: (t + n, 0))
    piece = pl.BlockSpec((1, PR, C), lambda t, j: (t * steps + j, 0, 0))
    return pl.pallas_call(
        last_kernel,
        grid=(n, steps),
        in_specs=[tile, tile, pl.BlockSpec((1, S, Q, 2 * RD, C), lambda t, j: (0, 0, j, 0, 0)), row, row, pl.BlockSpec((T, D), lambda t, j: (t, 0))]
        + [piece] * 4,
        out_specs=[pl.BlockSpec((2, T, D), lambda t, j: (0, t, 0))] + [hbm] * 3,
        out_shape=[jax.ShapeDtypeStruct((2, TOK // 2, D), bf16)] + [jax.ShapeDtypeStruct((L, RD, FF), bf16)] * 2 + [jax.ShapeDtypeStruct((L, RF, D), bf16)],
        scratch_shapes=[pltpu.VMEM((T, D), f32), pltpu.VMEM((2, L, PR, C), bf16), pltpu.SemaphoreType.DMA((2, L))],
        compiler_params=pltpu.CompilerParams(vmem_limit_bytes=VM),
        cost_estimate=pl.CostEstimate(flops=2 * TOK * D * FF, bytes_accessed=150 << 20, transcendentals=0),
        name="last_pass",
    )(dgs, dus, whole, h, dy, begun, s1, t1, s0, t0)


def transposed_kernel(x, y):
    y[...] = x[...].T


def transposed(x):
    T = 512
    return pl.pallas_call(
        transposed_kernel,
        grid=(TOK // T,),
        in_specs=[pl.BlockSpec((T, D), lambda i: (i, 0))],
        out_specs=pl.BlockSpec((D, T), lambda i: (0, i)),
        out_shape=jax.ShapeDtypeStruct((D, TOK), bf16),
        name="transposed",
    )(x)


def solution(mesh):
    def step(x, dy, wg, wu, wd):
        x, dy = x[0], dy[0]
        a0, a0t, whole = prep(x, wg, wu, wd)
        dyt = transposed(dy)
        h1, a1, a1t, gs, us, whole = forward(a0, x, whole)
        sums1, theirs1, kept, out_a, dgs, dus, whole = weights_pass(False, a1, a1t, dy, dyt, whole)
        by1, by1t, sums1, theirs1 = input_pass(1, dgs, dus, whole, h1, dy, sums1, theirs1, kept, out_a)
        sums0, theirs0, kept, out_a, dgs, dus = weights_pass(True, None, a0t, by1, by1t, whole, gs, us)
        begun, sums0, theirs0 = input_pass(0, dgs, dus, whole, x, by1, sums0, theirs0, kept, out_a)
        by0, *grads = last_pass(dgs, dus, whole, x, by1, begun, sums1, theirs1, sums0, theirs0)
        return (by0.reshape(1, TOK, D), *grads)

    states, cut = P(("rep", "r", "s"), None, None), P(None, "s", None)
    return jax.shard_map(
        step,
        mesh=mesh,
        in_specs=(states, states) + (cut,) * 3,
        out_specs=(states,) + (P("rep", "s", None),) * 3,
        check_vma=False,
    )
```

```python
import functools

import jax
import jax.numpy as jnp
from jax import lax
from jax.experimental import pallas as pl
from jax.experimental.pallas import tpu as pltpu
from jax.sharding import PartitionSpec as P

f32, bf16 = jnp.float32, jnp.bfloat16
TOK, D, FF, L = 4096, 768, 6144, 2
S = 4
C = 512
J = FF // C
LAST = J - 1
W = C // S
RD, RF = D // S, FF // S
PR = 2 * RD + W * D // C
HALF = PR // 2
EARLY = 2
VM = 67043328
MESH = pl.DeviceIdType.MESH
once = pl.Buffered(1)
hbm = pl.BlockSpec(memory_space=pl.ANY)


def dot(a, b, ca=1, cb=0):
    return lax.dot_general(a, b, (((ca,), (cb,)), ((), ())), preferred_element_type=f32)


def dot_across(a, b):
    return dot(a, b, 1, 1)


def params(matmuls, mib, **more):
    return dict(
        compiler_params=pltpu.CompilerParams(vmem_limit_bytes=VM, **more),
        cost_estimate=pl.CostEstimate(flops=2 * matmuls * TOK * D * FF, bytes_accessed=mib << 20, transcendentals=0),
    )


def place_in_grid():
    return pl.program_id(0), pl.program_id(1)


def normed(wide):
    scale = lax.rsqrt(jnp.mean(wide**2, -1, keepdims=True) + 1e-6)
    return (wide * scale).astype(bf16)


def norm_back(by, h, dy):
    by, wide = by.astype(bf16).astype(f32), h.astype(f32)
    scale = lax.rsqrt(jnp.mean(wide**2, -1, keepdims=True) + 1e-6)
    along = jnp.sum(by * wide, -1, keepdims=True) / D
    by_h = (by * scale - wide * (scale * scale * scale * along)).astype(bf16)
    return (dy.astype(f32) + by_h.astype(f32)).astype(bf16)


def gate_of(w):
    return jnp.concatenate([w[s, 0:RD, :] for s in range(S)], axis=0)


def up_of(w):
    return jnp.concatenate([w[s, RD : 2 * RD, :] for s in range(S)], axis=0)


def down_of(w, at=2 * RD):
    def rows(s):
        fold = jnp.concatenate([w[s, at + W : at + W + W // 2, 0 : D - C], w[s, at + W : at + W + W // 2, D - C : 2 * (D - C)]], axis=0)
        return jnp.concatenate([w[s, at : at + W, :], fold], axis=1)

    return jnp.concatenate([rows(s) for s in range(S)], axis=0)


def piece_slices(j):
    for s in range(S):
        cols = pl.ds(pl.multiple_of(RF * s + W * j, W), W)
        yield 0, (pl.ds(0, RD), cols), (pl.ds(0, RD), pl.ds(W * s, W))
        yield 1, (pl.ds(0, RD), cols), (pl.ds(RD, RD), pl.ds(W * s, W))
    at = pl.multiple_of(W * j, W)
    yield 2, (pl.ds(at, W), pl.ds(0, C)), (pl.ds(2 * RD, W), pl.ds(0, C))
    yield 2, (pl.ds(at, W // 2), pl.ds(C, D - C)), (pl.ds(2 * RD + W, W // 2), pl.ds(0, D - C))
    yield 2, (pl.ds(at + W // 2, W // 2), pl.ds(C, D - C)), (pl.ds(2 * RD + W, W // 2), pl.ds(D - C, D - C))


def place():
    me, y = lax.axis_index("s"), lax.axis_index("r")
    return me, y, {"s": me + 1 - 2 * lax.rem(me, 2)}, {"s": lax.rem(me + 2, S)}, {"r": 1 - y}


def greet():
    _, _, core, across, copy = place()
    barrier = pltpu.get_barrier_semaphore()
    for to in (core, across, copy):
        pl.semaphore_signal(barrier, inc=1, device_id=to, device_id_type=MESH)
    pl.semaphore_wait(barrier, 3)


def remote(src, dst, send, recv, to):
    return pltpu.make_async_remote_copy(src_ref=src, dst_ref=dst, send_sem=send, recv_sem=recv, device_id=to, device_id_type=MESH)


FROM = (0, 1, 2, 0, 0)


def wait_pieces(whole, n, sem):
    ref = whole.at[0, pl.ds(0, n), 0]
    pltpu.make_async_copy(ref, ref, sem).wait()


class Gather:
    def __init__(self, first, mine, whole, stage, send, recv, local):
        self.first, self.mine, self.whole, self.stage = first, mine, whole, stage
        self.send, self.recv, self.local, self.ring = send, recv, local, stage.shape[0]

    @staticmethod
    def scratch(n, ring):
        return [
            pltpu.VMEM((ring, PR, C), bf16),
            pltpu.SemaphoreType.DMA((ring,)),
            pltpu.SemaphoreType.DMA((n, 3)),
            pltpu.SemaphoreType.DMA((ring, 2)),
        ]

    def copy(self, k, n):
        me, y, core, across, copy = place()
        l, j, slot = k // J, lax.rem(k, J), lax.rem(k, self.ring)
        near, far = pl.ds(pl.multiple_of(HALF * y, HALF), HALF), pl.ds(pl.multiple_of(HALF * (1 - y), HALF), HALF)
        rows = ((), (near,), (near,), (near,), (far,))[n]
        s = me if n < 2 else lax.rem(me + 2, S)
        what = self.whole.at[(l, s, j, *rows)]
        src = self.stage.at[(slot, *rows)] if n < 2 else what
        return remote(src, what, self.send.at[slot], self.recv.at[k - self.first, FROM[n]], (core, across, copy, core, core)[n])

    def keep(self, k):
        slot = lax.rem(k, self.ring)
        return pltpu.make_async_copy(self.stage.at[slot], self.whole.at[k // J, place()[0], lax.rem(k, J)], self.local.at[slot, 1])

    def pack(self, k):
        slot = lax.rem(k, self.ring)
        for m, src, dst in piece_slices(lax.rem(k, J)):
            pltpu.make_async_copy(self.mine[m].at[(k // J, *src)], self.stage.at[(slot, *dst)], self.local.at[slot, 0]).start()

    def start(self, k):
        slot = lax.rem(k, self.ring)
        pltpu.make_async_copy(self.stage.at[slot], self.stage.at[slot], self.local.at[slot, 0]).wait()
        self.copy(k, 1).start()
        self.copy(k, 0).start()
        self.keep(k).start()

    def across(self, k):
        self.copy(k, 1).wait_recv()
        self.copy(k, 2).start()
        self.copy(k, 3).start()

    def along(self, k):
        self.copy(k, 2).wait_recv()
        self.copy(k, 4).start()

    def finish(self, k):
        wait_pieces(self.whole, 2, self.recv.at[k - self.first, 0])
        wait_pieces(self.whole, 3, self.send.at[lax.rem(k, self.ring)])
        self.keep(k).wait()


def fetch(whole, held, sem, l, j):
    slot = lax.rem(j, 2)
    return pltpu.make_async_copy(whole.at[l, :, j], held.at[slot], sem.at[slot])


SWIFT = 2
PARTS = 3
ALL, SOON, LATE = (0, PARTS), (0, PARTS - 1), (PARTS - 1, PARTS)


class Swift(Gather):
    def __init__(self, mine, whole, held, send, recv, local):
        self.mine, self.whole, self.held, self.send, self.recv, self.local = mine, whole, held, send, recv, local

    SCRATCH = [pltpu.SemaphoreType.DMA((SWIFT,)), pltpu.SemaphoreType.DMA((SWIFT, 3, PARTS)), pltpu.SemaphoreType.DMA((SWIFT, 2))]

    def copies(self, k, n, parts=ALL):
        me, y, core, across, copy = place()
        s = me if n < 2 else lax.rem(me + 2, S)
        to = (core, across, copy, core, core)[n]
        for i in range(*parts) if n else (0,):
            rows = HALF * (1 - y if n == 4 else y) + HALF // PARTS * i
            what = self.held.at[(k, s, pl.ds(pl.multiple_of(rows, HALF // PARTS), HALF // PARTS)) if n else (k, s)]
            yield remote(what, what, self.send.at[k], self.recv.at[k, FROM[n], i if FROM[n] else 0], to)

    def keep(self, k):
        return pltpu.make_async_copy(self.held.at[k], self.whole.at[0, :, k], self.local.at[k, 1])

    def pack(self, k):
        for m, src, dst in piece_slices(k):
            pltpu.make_async_copy(self.mine[m].at[(0, *src)], self.held.at[(k, place()[0], *dst)], self.local.at[k, 0]).start()

    def start(self, k):
        own = self.held.at[k, place()[0]]
        pltpu.make_async_copy(own, own, self.local.at[k, 0]).wait()
        for n in (1, 0):
            for copy in self.copies(k, n):
                copy.start()

    def across(self, k, parts=ALL):
        for x, y, core in zip(*(self.copies(k, n, parts) for n in (1, 2, 3))):
            x.wait_recv()
            y.start()
            core.start()

    def along(self, k, parts=ALL):
        for y, core in zip(*(self.copies(k, n, parts) for n in (2, 4))):
            y.wait_recv()
            core.start()

    def finish(self, k):
        wait_pieces(self.whole, 2, self.recv.at[k, 0, 0])
        wait_pieces(self.whole, 3, self.send.at[k])
        self.keep(k).start()


def rows_of(t, T):
    return pl.ds(pl.multiple_of(t * T, T), T)


def in_turn(low, high, f):
    def body(i, _):
        f(i)
        return 0

    lax.fori_loop(low, high, body, 0)


def by_rows(low, high, f):
    n = 256
    in_turn(low // n, high // n, lambda i: f(rows_of(i, n)))


def forward_kernel(T, x_i, wg, wu, wd, h_o, a0_o, a1_o, gs, us, whole, x, a, acc, held, load, io, first, *rest):
    j, t = place_in_grid()
    swift = Swift((wg, wu, wd), whole, held, *rest[:3])
    gather = Gather(SWIFT, (wg, wu, wd), whole, *rest[3:])
    ahead, K, NT = 4, J + EARLY, TOK // T
    assert NT == 2 and SWIFT == 2 and EARLY == 2
    rows = pl.ds(pl.multiple_of(t * T, T), T)

    def outs(t):
        part = pl.ds(pl.multiple_of(t * T, T), T)
        return [pltpu.make_async_copy(x.at[part], h_o.at[part], io.at[1, t]), pltpu.make_async_copy(a.at[part], a1_o.at[part], io.at[2, t])]

    def take(j):
        fetch(whole, held, load, 0, j).start()

    @pl.when((j == 0) & (t == 0))
    def _():
        n = 4
        states = lambda i: pltpu.make_async_copy(x_i.at[rows_of(i, TOK // n)], x.at[rows_of(i, TOK // n)], first.at[i])
        swift.pack(0)
        states(0).start()
        swift.pack(1)
        for i in range(1, n):
            states(i).start()
        greet()
        for k in range(SWIFT):
            swift.start(k)
        in_turn(SWIFT, ahead + 2, gather.pack)

        def norm(i):
            states(i).wait()

            def some(rows):
                a[rows, :] = normed(x[rows, :].astype(f32))

            by_rows(TOK // n * i, TOK // n * (i + 1), some)

        norm(0)
        swift.across(0)
        gather.start(SWIFT)
        in_turn(1, n, norm)
        pltpu.make_async_copy(a, a0_o, io.at[0, 1]).start()
        swift.along(0)
        in_turn(SWIFT + 1, ahead + 1, gather.start)
        swift.across(1, SOON)
        swift.finish(0)

    @pl.when((t == 0) & (j > 0))
    def _():
        @pl.when(j == 1)
        def _():
            swift.along(1, LATE)
            swift.finish(1)

        @pl.when(j >= SWIFT)
        def _():
            fetch(whole, held, load, 0, j).wait()

            gather.along(j + 1)

        @pl.when(j < LAST)
        def _():
            gather.across(j + 2)

        @pl.when(j == LAST)
        def _():
            gather.along(J + 1)

        @pl.when(j + ahead < K)
        def _():
            gather.start(j + ahead)

        @pl.when(j + ahead + 1 < K)
        def _():
            gather.pack(j + ahead + 1)

    @pl.when(t == 1)
    def _():
        @pl.when(j == 0)
        def _():
            swift.across(1, LATE)
            swift.along(1, SOON)
            gather.across(SWIFT)

        @pl.when(j == 1)
        def _():
            gather.along(2)

        @pl.when(j > 0)
        def _():
            gather.finish(j + 1)

        @pl.when((j == 1) | (j == 2))
        def _():
            swift.keep(j - 1).wait()

        @pl.when((j > 0) & (j + 1 < J))
        def _():
            take(j + 1)

        @pl.when(j == J - 2)
        def _():
            gather.across(J + 1)

        @pl.when(j == LAST)
        def _():
            gather.finish(J + 1)

    w = held.at[lax.rem(j, 2)]
    lhs = a[rows, :]
    g, u = dot(lhs, gate_of(w)), dot(lhs, up_of(w))
    gs[0], us[0] = g, u
    act = (g * jax.nn.sigmoid(g) * u).astype(bf16)
    acc[rows, :] = jnp.where(j == 0, 0.0, acc[rows, :]) + dot(act, down_of(w))

    @pl.when(j == LAST)
    def _():
        @pl.when(t == 0)
        def _():
            pltpu.make_async_copy(a, a0_o, io.at[0, 1]).wait()

        def some(rows):
            h = (x[rows, :].astype(f32) + acc[rows, :].astype(bf16).astype(f32)).astype(bf16)
            x[rows, :] = h
            a[rows, :] = normed(h.astype(f32))

        by_rows(t * T, (t + 1) * T, some)
        for copy in outs(t):
            copy.start()

        @pl.when(t == NT - 1)
        def _():
            for i in range(NT):
                for copy in outs(i):
                    copy.wait()


def forward(x, wg, wu, wd):
    T = 2048
    tile = pl.BlockSpec((1, T, C), lambda j, t: (j, t, 0))
    states = jax.ShapeDtypeStruct((TOK, D), bf16)
    return pl.pallas_call(
        functools.partial(forward_kernel, T),
        grid=(J, TOK // T),
        in_specs=[hbm] * 4,
        out_specs=[hbm] * 3 + [tile, tile, hbm],
        out_shape=[states] * 3 + [jax.ShapeDtypeStruct((J, TOK, C), f32)] * 2 + [jax.ShapeDtypeStruct((L, S, J, PR, C), bf16)],
        scratch_shapes=[
            pltpu.VMEM((TOK, D), bf16),
            pltpu.VMEM((TOK, D), bf16),
            pltpu.VMEM((TOK, D), f32),
            pltpu.VMEM((2, S, PR, C), bf16),
            pltpu.SemaphoreType.DMA((2,)),
            pltpu.SemaphoreType.DMA((3, 2)),
            pltpu.SemaphoreType.DMA((4,)),
        ]
        + Swift.SCRATCH
        + Gather.scratch(J + EARLY - SWIFT, 6),
        **params(3, 250, collective_id=0, has_side_effects=True),
        name="forward",
    )(x, wg, wu, wd)


def pack(s, ag, au, ad):
    rows, down = pl.ds(pl.multiple_of(RD * s, RD), RD), pl.multiple_of(W * s, W)
    yield slice(0, RD), slice(0, C), ag[rows, :]
    yield slice(RD, 2 * RD), slice(0, C), au[rows, :]
    yield slice(2 * RD, 2 * RD + W), slice(0, C), ad[pl.ds(down, W), :C]
    yield slice(2 * RD + W, PR), slice(0, D - C), ad[pl.ds(down, W // 2), C:]
    yield slice(2 * RD + W, PR), slice(D - C, C), ad[pl.ds(down + W // 2, W // 2), C:]


class Reduce:
    def __init__(self, sums, theirs, kept, out_a, in_a, kept_b, out_b, in_b, out_c, sems):
        self.sums, self.theirs = sums, theirs
        self.kept, self.out_a, self.in_a = kept, out_a, in_a
        self.kept_b, self.out_b, self.in_b, self.out_c = kept_b, out_b, in_b, out_c
        self.sems = sems

    SCRATCH = [
        pltpu.VMEM((2, PR, C), f32),
        pltpu.VMEM((2, PR, C), bf16),
        pltpu.VMEM((2, 2, PR, C), bf16),
        pltpu.VMEM((PR, C), f32),
        pltpu.VMEM((PR, C), bf16),
        pltpu.VMEM((2, PR, C), bf16),
        pltpu.VMEM((PR, C), bf16),
        pltpu.SemaphoreType.DMA((3, 4)),
    ]

    def at(self, sums, theirs):
        return Reduce(sums, theirs, self.kept, self.out_a, self.in_a, self.kept_b, self.out_b, self.in_b, self.out_c, self.sems)

    def copy_a(self, j, src=None):
        slot = lax.rem(j, 2)
        return remote(self.out_a if src is None else src, self.in_a.at[slot], self.sems.at[0, 0], self.sems.at[0, 1 + slot], place()[2])

    def copy_b(self, j):
        slot = lax.rem(j, 2)
        return remote(self.out_b, self.in_b.at[slot], self.sems.at[1, 0], self.sems.at[1, 1 + slot], place()[3])

    def copy_c(self, j):
        return remote(self.out_c, self.theirs.at[j], self.sems.at[2, 0], self.sems.at[2, 1 + lax.rem(j, 2)], place()[4])

    def store_c(self, j):
        return pltpu.make_async_copy(self.out_c, self.sums.at[j], self.sems.at[2, 3])

    def again_c(self, j, send, recv):
        return remote(self.sums.at[j], self.theirs.at[j], send, recv, place()[4])

    def collect(self, ag, au, ad):
        c = lax.rem(lax.axis_index("s"), 2)
        for x in range(2):
            for r, cols, v in pack(2 * x + 1 - c, ag, au, ad):
                self.out_a[x, r, cols] = v.astype(bf16)
            for r, cols, v in pack(2 * x + c, ag, au, ad):
                self.kept[x, r, cols] = v

    def step_a(self, j):
        self.copy_a(j).wait()
        slot, x = lax.rem(j, 2), lax.axis_index("s") // 2
        self.out_b[...] = (self.kept[1 - x] + self.in_a[slot, 1 - x].astype(f32)).astype(bf16)
        self.copy_b(j).start()
        self.kept_b[...] = self.kept[x] + self.in_a[slot, x].astype(f32)

    def step_b(self, j, send=True):
        self.copy_b(j).wait()
        self.out_c[...] = (self.kept_b[...] + self.in_b[lax.rem(j, 2)].astype(f32)).astype(bf16)
        if send:
            self.copy_c(j).start()
        self.store_c(j).start()

    def step_c(self, j):
        self.copy_c(j).wait()
        self.store_c(j).wait()

    def follow(self, j):
        for stage, step in ((3, self.step_c), (2, self.step_b), (1, self.step_a)):
            pl.when(j >= stage)(functools.partial(step, j - stage))

    def handed(self, kept, out_a, sems):
        return [pltpu.make_async_copy(src, dst, sems.at[i]) for i, (src, dst) in enumerate(((self.kept, kept), (self.out_a, out_a)))]

    def leave(self, copies):
        self.step_c(J - 3)
        self.step_b(J - 2, send=False)
        self.store_c(J - 2).wait()
        for copy in copies:
            copy.wait()


def gradients(by, g, u):
    sig = jax.nn.sigmoid(g)
    silu = g * sig
    return (silu * u).astype(bf16), (by * u * (sig + silu * (1 - sig))).astype(bf16), (by * silu).astype(bf16)


def accumulate(t, a, dy, act, dg, du, ag, au, ad):
    for acc, l, r in ((ag, a, dg), (au, a, du), (ad, act, dy)):
        acc[...] = jnp.where(t == 0, 0.0, acc[...]) + dot(l, r, 0, 0)


PIECE = 512


class Pair:
    def __init__(self, *copies):
        self.copies = copies

    def start(self):
        for copy in self.copies:
            copy.start()

    def wait(self):
        for copy in self.copies:
            copy.wait()


def state_copies(i, first, second, sems):
    rows = rows_of(i, PIECE)
    return Pair(*(pltpu.make_async_copy(src.at[rows], dst.at[rows], sems.at[n, i]) for n, (src, dst) in enumerate((first, second))))


def second_kernel(a_i, dy_i, h, wg, wu, wd, _, out, sums, theirs, kept_o, out_o, whole, a, dy, ag, au, ad, total, held, load, save, states, *rest):
    j, t = place_in_grid()
    NT = 4
    T = TOK // NT
    gather = Gather(J + EARLY, (wg, wu, wd), whole, *rest[:4])
    reduce = Reduce(sums, theirs, *rest[4:])
    lead = EARLY + 1
    rows = rows_of(t, T)

    parts = T // PIECE

    def inputs(i):
        return state_copies(i, (a_i, a), (dy_i, dy), states)

    def layer_input(i):
        return pltpu.make_async_copy(h.at[rows_of(i, PIECE)], a.at[rows_of(i, PIECE)], states.at[0, i])

    def result(i):
        return pltpu.make_async_copy(dy.at[rows_of(i, PIECE)], out.at[rows_of(i, PIECE)], states.at[1, i])

    @pl.when((j == 0) & (t == 0))
    def _():
        in_turn(J + EARLY, J + lead + 1, gather.pack)
        fetch(whole, held, load, 1, 0).start()
        in_turn(0, NT * parts, lambda i: inputs(i).start())
        greet()
        gather.start(J + EARLY)

    @pl.when(j == 0)
    def _():
        in_turn(parts * t, parts * (t + 1), lambda i: inputs(i).wait())

    @pl.when(t == 0)
    def _():
        fetch(whole, held, load, 1, j).wait()

        @pl.when((j + 1 >= EARLY) & (j + 1 < J))
        def _():
            gather.along(J + j + 1)

        @pl.when(j + lead < J)
        def _():
            gather.start(J + j + lead)

        @pl.when(j + lead + 1 < J)
        def _():
            gather.pack(J + j + lead + 1)

    @pl.when(t == 1)
    def _():
        reduce.follow(j)

    @pl.when((t == 2) & (j + 2 < J))
    def _():
        gather.across(J + j + 2)

    @pl.when((t == 3) & (j + 1 < J))
    def _():
        @pl.when(j + 1 >= EARLY)
        def _():
            gather.finish(J + j + 1)

        fetch(whole, held, load, 1, j + 1).start()

    w = held.at[lax.rem(j, 2)]
    lhs, ct = a[rows, :], dy[rows, :]
    gate, up = gate_of(w), up_of(w)
    g, u = dot(lhs, gate), dot(lhs, up)
    by = dot_across(ct, down_of(w)).astype(bf16).astype(f32)
    act, dg, du = gradients(by, g, u)
    accumulate(t, lhs, ct, act, dg, du, ag, au, ad)
    total[rows, :] = jnp.where(j == 0, 0.0, total[rows, :]) + (dot_across(dg, gate) + dot_across(du, up))

    @pl.when(t == NT - 1)
    def _():
        reduce.collect(ag, au, ad)

        @pl.when(j < LAST)
        def _():
            reduce.copy_a(j).start()

    @pl.when(j == LAST)
    def _():
        in_turn(parts * t, parts * (t + 1), lambda i: layer_input(i).start())

        @pl.when(t == NT - 1)
        def _():
            copies = reduce.handed(kept_o, out_o, save)
            for copy in copies:
                copy.start()

            def back(i):
                layer_input(i).wait()

                def some(rows):
                    dy[rows, :] = norm_back(total[rows, :], a[rows, :], dy[rows, :])

                by_rows(i * PIECE, (i + 1) * PIECE, some)
                result(i).start()

            in_turn(0, NT * parts, back)
            reduce.leave(copies)
            in_turn(0, NT * parts, lambda i: result(i).wait())


PIECES = jax.ShapeDtypeStruct((J, PR, C), bf16)


def second_pass(a, dy, h, wg, wu, wd, whole):
    T = TOK // 4
    return pl.pallas_call(
        second_kernel,
        grid=(J, TOK // T),
        in_specs=[hbm] * 7,
        out_specs=[hbm] * 6,
        out_shape=[jax.ShapeDtypeStruct((TOK, D), bf16), PIECES, PIECES]
        + [jax.ShapeDtypeStruct((2, PR, C), f32), jax.ShapeDtypeStruct((2, PR, C), bf16), jax.ShapeDtypeStruct((L, S, J, PR, C), bf16)],
        scratch_shapes=[
            pltpu.VMEM((TOK, D), bf16),
            pltpu.VMEM((TOK, D), bf16),
            pltpu.VMEM((D, C), f32),
            pltpu.VMEM((D, C), f32),
            pltpu.VMEM((C, D), f32),
            pltpu.VMEM((TOK, D), f32),
            pltpu.VMEM((2, S, PR, C), bf16),
            pltpu.SemaphoreType.DMA((2,)),
            pltpu.SemaphoreType.DMA((2,)),
            pltpu.SemaphoreType.DMA((2, TOK // PIECE)),
        ]
        + Gather.scratch(J - EARLY, 4)
        + Reduce.SCRATCH,
        input_output_aliases={6: 5},
        **params(8, 100, collective_id=1, has_side_effects=True),
        name="second_pass",
    )(a, dy, h, wg, wu, wd, whole)


def first_kernel(a_i, dy_i, w, gs, us, s1_i, t1_i, kept_i, out_i, dgs, dus, sums, theirs, kept_o, out_o, s1, t1, a, dy, ag, au, ad, save, states, *rest):
    j, t = place_in_grid()
    T = dgs.shape[1]
    NT = TOK // T
    rows = rows_of(t, T)
    reduce = Reduce(sums, theirs, *rest)
    before = reduce.at(s1, t1)
    kept = lambda: pltpu.make_async_copy(kept_i, reduce.kept, save.at[0])
    again = lambda: before.again_c(J - 2, save.at[1], save.at[2])

    parts = T // PIECE

    def inputs(i):
        return state_copies(i, (a_i, a), (dy_i, dy), states)

    @pl.when((j == 0) & (t == 0))
    def _():
        in_turn(0, parts, lambda i: inputs(i).start())
        kept().start()
        in_turn(parts, NT * parts, lambda i: inputs(i).start())
        greet()
        before.copy_a(LAST, out_i).start()
        again().start()

    @pl.when(j == 0)
    def _():
        in_turn(parts * t, parts * (t + 1), lambda i: inputs(i).wait())

    @pl.when(t == 1)
    def _():
        @pl.when(j == 2)
        def _():
            before.step_c(LAST)

        @pl.when(j == 1)
        def _():
            again().wait()
            before.step_b(LAST)

        @pl.when(j == 0)
        def _():
            kept().wait()
            before.step_a(LAST)

        reduce.follow(j)

    lhs, ct = a[rows, :], dy[rows, :]
    by = dot_across(ct, down_of(w.at[0, :, 0], 0)).astype(bf16).astype(f32)
    act, dg, du = gradients(by, gs[0], us[0])
    dgs[0], dus[0] = dg, du
    accumulate(t, lhs, ct, act, dg, du, ag, au, ad)

    @pl.when(t == NT - 1)
    def _():
        reduce.collect(ag, au, ad)

        @pl.when(j < LAST)
        def _():
            reduce.copy_a(j).start()

        @pl.when(j == LAST)
        def _():
            copies = reduce.handed(kept_o, out_o, save)
            for copy in copies:
                copy.start()
            reduce.leave(copies)


def first_pass(a, dy, whole, gs, us, s1, t1, kept, out_a):
    T = 1024
    tile = pl.BlockSpec((1, T, C), lambda j, t: (j, t, 0))
    return pl.pallas_call(
        first_kernel,
        grid=(J, TOK // T),
        in_specs=[hbm, hbm, pl.BlockSpec((1, S, 1, PR - 2 * RD, C), lambda j, t: (0, 0, j, 2, 0)), tile, tile] + [hbm] * 4,
        out_specs=[tile, tile] + [hbm] * 6,
        out_shape=[jax.ShapeDtypeStruct((J, TOK, C), bf16)] * 2
        + [PIECES, PIECES, jax.ShapeDtypeStruct((2, PR, C), f32), jax.ShapeDtypeStruct((2, PR, C), bf16), PIECES, PIECES],
        scratch_shapes=[
            pltpu.VMEM((TOK, D), bf16),
            pltpu.VMEM((TOK, D), bf16),
            pltpu.VMEM((D, C), f32),
            pltpu.VMEM((D, C), f32),
            pltpu.VMEM((C, D), f32),
            pltpu.SemaphoreType.DMA((3,)),
            pltpu.SemaphoreType.DMA((2, TOK // PIECE)),
        ]
        + Reduce.SCRATCH,
        input_output_aliases={5: 6, 6: 7},
        **params(4, 300, collective_id=2, has_side_effects=True),
        name="first_pass",
    )(a, dy, whole, gs, us, s1, t1, kept, out_a)


PART = TOK // 2


Q = 2
STEPS = J // Q
END = STEPS - 1


def contract(j, dgs, dus, w, acc):
    n = PART // Q
    for i in range(PART // n):
        rows = slice(i * n, (i + 1) * n)
        total = jnp.where(j == 0, 0.0, acc[rows, :])
        for q in range(Q):
            held = w.at[0, :, q]
            total = total + (dot_across(dgs[q, rows], gate_of(held)) + dot_across(dus[q, rows], up_of(held)))
        acc[rows, :] = total


def input_kernel(dgs, dus, w, h_i, dy_i, s1, t1, s_i, t_i, kept_i, out_i, g1, out, sums, theirs, acc, h, dy, save, states, *rest):
    reduce = Reduce(sums, theirs, *rest)
    j = pl.program_id(0)
    late_states(0, j, h_i, dy_i, h, dy, states)

    @pl.when(j == 0)
    def _():
        pltpu.make_async_copy(kept_i, reduce.kept, save.at[0]).start()
        greet()
        reduce.copy_a(LAST, out_i).start()
        reduce.again_c(J - 2, save.at[1], save.at[2]).start()

    @pl.when(j == 1)
    def _():
        pltpu.make_async_copy(kept_i, reduce.kept, save.at[0]).wait()
        reduce.step_a(LAST)

    @pl.when(j == 3)
    def _():
        reduce.step_b(LAST)

    @pl.when(j == END)
    def _():
        reduce.again_c(J - 2, save.at[1], save.at[2]).wait()
        reduce.step_c(LAST)

    g1[...] = (s1[...].astype(f32) + t1[...].astype(f32)).astype(bf16)
    contract(j, dgs, dus, w, acc)

    @pl.when(j == END)
    def _():
        def some(rows):
            out[rows, :] = norm_back(acc[rows, :], h[rows, :], dy[rows, :])

        by_rows(0, PART, some)


def late_states(part, j, h_i, dy_i, h, dy, sems):
    copies = lambda: [pltpu.make_async_copy(src.at[pl.ds(part * PART, PART)], dst, sems.at[i]) for i, (src, dst) in enumerate(((h_i, h), (dy_i, dy)))]

    @pl.when(j == 2)
    def _():
        for copy in copies():
            copy.start()

    @pl.when(j == END)
    def _():
        for copy in copies():
            copy.wait()


STATES = [pltpu.VMEM((PART, D), f32), pltpu.VMEM((PART, D), bf16), pltpu.VMEM((PART, D), bf16)]
piece = pl.BlockSpec((Q, PR, C), lambda j: (j, 0, 0))


def part_specs(part):
    tile = pl.BlockSpec((Q, PART, C), lambda j: (j, part, 0))
    return [tile, tile, pl.BlockSpec((1, S, Q, 2 * RD, C), lambda j: (0, 0, j, 0, 0)), hbm, hbm]


def input_pass(dgs, dus, whole, h, dy, s1, t1, sums, theirs, kept, out_a):
    return pl.pallas_call(
        input_kernel,
        grid=(STEPS,),
        in_specs=part_specs(0) + [piece, piece] + [hbm] * 4,
        out_specs=[piece, pl.BlockSpec((PART, D), lambda j: (0, 0), pipeline_mode=once), hbm, hbm],
        out_shape=[PIECES, jax.ShapeDtypeStruct((PART, D), bf16), PIECES, PIECES],
        scratch_shapes=STATES + [pltpu.SemaphoreType.DMA((3,)), pltpu.SemaphoreType.DMA((2,))] + Reduce.SCRATCH,
        input_output_aliases={7: 2, 8: 3},
        **params(1, 100, collective_id=3, has_side_effects=True),
        name="input_pass",
    )(dgs, dus, whole, h, dy, s1, t1, sums, theirs, kept, out_a)


def last_kernel(dgs, dus, w, h_i, dy_i, g1, s0, t0, begun, out, og, ou, od, acc, h, dy, stage, passing, sems, io, states):
    j = pl.program_id(0)
    late_states(1, j, h_i, dy_i, h, dy, states)
    slot = lax.rem(j, 2)
    first = lambda: pltpu.make_async_copy(begun, passing, io.at[0])
    second = lambda: pltpu.make_async_copy(passing, out.at[0], io.at[1])

    def wait(slot):
        for l in range(L):
            pltpu.make_async_copy(stage.at[slot, l], stage.at[slot, l], sems.at[slot, l]).wait()

    @pl.when(j == 0)
    def _():
        first().start()

    @pl.when(j == 2)
    def _():
        first().wait()
        second().start()

    @pl.when(j >= 2)
    def _():
        wait(slot)

    stage[slot, 0] = (s0[...].astype(f32) + t0[...].astype(f32)).astype(bf16)
    stage[slot, 1] = g1[...]
    contract(j, dgs, dus, w, acc)
    for l in range(L):

        def unpack(q):
            for m, dst, src in piece_slices(Q * j + q):
                pltpu.make_async_copy(stage.at[(slot, l, q, *src)], (og, ou, od)[m].at[(l, *dst)], sems.at[slot, l]).start()

        in_turn(0, Q, unpack)

    @pl.when(j == END)
    def _():
        n = 4
        result = lambda i: pltpu.make_async_copy(dy.at[rows_of(i, PART // n)], out.at[1, rows_of(i, PART // n)], io.at[2 + i])

        def quarter(i):
            def some(rows):
                dy[rows, :] = norm_back(acc[rows, :], h[rows, :], dy[rows, :])

            by_rows(PART // n * i, PART // n * (i + 1), some)
            result(i).start()

        in_turn(0, n, quarter)
        wait(1 - slot)
        wait(slot)
        second().wait()
        in_turn(0, n, lambda i: result(i).wait())


def last_pass(dgs, dus, whole, h, dy, g1, s0, t0, begun):
    return pl.pallas_call(
        last_kernel,
        grid=(STEPS,),
        in_specs=part_specs(1) + [piece] * 3 + [hbm],
        out_specs=[hbm] * 4,
        out_shape=[jax.ShapeDtypeStruct((2, PART, D), bf16)] + [jax.ShapeDtypeStruct((L, RD, FF), bf16)] * 2 + [jax.ShapeDtypeStruct((L, RF, D), bf16)],
        scratch_shapes=STATES
        + [
            pltpu.VMEM((2, L, Q, PR, C), bf16),
            pltpu.VMEM((PART, D), bf16),
            pltpu.SemaphoreType.DMA((2, L)),
            pltpu.SemaphoreType.DMA((6,)),
            pltpu.SemaphoreType.DMA((2,)),
        ],
        **params(1, 150),
        name="last_pass",
    )(dgs, dus, whole, h, dy, g1, s0, t0, begun)


def solution(mesh):
    def step(x, dy, *weights):
        x, dy = x[0], dy[0]
        h1, a0, a1, gs, us, whole = forward(x, *weights)
        by1, s1, t1, kept, out_a, whole = second_pass(a1, dy, h1, *weights, whole)
        dgs, dus, s0, t0, kept, out_a, s1, t1 = first_pass(a0, by1, whole, gs, us, s1, t1, kept, out_a)
        g1, begun, s0, t0 = input_pass(dgs, dus, whole, x, by1, s1, t1, s0, t0, kept, out_a)
        by0, *grads = last_pass(dgs, dus, whole, x, by1, g1, s0, t0, begun)
        return (by0.reshape(1, TOK, D), *grads)

    states, cut = P(("rep", "r", "s"), None, None), P(None, "s", None)
    return jax.shard_map(
        step,
        mesh=mesh,
        in_specs=(states, states) + (cut,) * 3,
        out_specs=(states,) + (P("rep", "s", None),) * 3,
        check_vma=False,
    )
```

```python
import functools

import jax
import jax.numpy as jnp
from jax import lax
from jax.experimental import pallas as pl
from jax.experimental.pallas import tpu as pltpu
from jax.sharding import PartitionSpec as P

f32, bf16 = jnp.float32, jnp.bfloat16
TOK, D, FF, L = 4096, 768, 6144, 2
S = 4
C = 512
J = FF // C
LAST = J - 1
W = C // S
RD, RF = D // S, FF // S
PR = 2 * RD + W * D // C
HALF = PR // 2
BLOCKS = 2
EARLY = 2
VM = 67043328
MESH = pl.DeviceIdType.MESH
once = pl.Buffered(1)
hbm = pl.BlockSpec(memory_space=pl.ANY)


def dot(a, b, ca=1, cb=0):
    return lax.dot_general(a, b, (((ca,), (cb,)), ((), ())), preferred_element_type=f32)


def dot_across(a, b):
    return dot(a, b, 1, 1)


def params(matmuls, mib, **more):
    return dict(
        compiler_params=pltpu.CompilerParams(vmem_limit_bytes=VM, **more),
        cost_estimate=pl.CostEstimate(flops=2 * matmuls * TOK * D * FF, bytes_accessed=mib << 20, transcendentals=0),
    )


def place_in_grid():
    return pl.program_id(0), pl.program_id(1)


def normed(wide):
    scale = lax.rsqrt(jnp.mean(wide**2, -1, keepdims=True) + 1e-6)
    return (wide * scale).astype(bf16)


def norm_back(by, h, dy):
    by, wide = by.astype(bf16).astype(f32), h.astype(f32)
    scale = lax.rsqrt(jnp.mean(wide**2, -1, keepdims=True) + 1e-6)
    along = jnp.sum(by * wide, -1, keepdims=True) / D
    by_h = (by * scale - wide * (scale * scale * scale * along)).astype(bf16)
    return (dy.astype(f32) + by_h.astype(f32)).astype(bf16)


def gate_of(w):
    return jnp.concatenate([w[s, 0:RD, :] for s in range(S)], axis=0)


def up_of(w):
    return jnp.concatenate([w[s, RD : 2 * RD, :] for s in range(S)], axis=0)


def down_of(w, at=2 * RD):
    def rows(s):
        fold = jnp.concatenate([w[s, at + W : at + W + W // 2, 0 : D - C], w[s, at + W : at + W + W // 2, D - C : 2 * (D - C)]], axis=0)
        return jnp.concatenate([w[s, at : at + W, :], fold], axis=1)

    return jnp.concatenate([rows(s) for s in range(S)], axis=0)


def piece_slices(j):
    for s in range(S):
        cols = pl.ds(pl.multiple_of(RF * s + W * j, W), W)
        yield 0, (pl.ds(0, RD), cols), (pl.ds(0, RD), pl.ds(W * s, W))
        yield 1, (pl.ds(0, RD), cols), (pl.ds(RD, RD), pl.ds(W * s, W))
    at = pl.multiple_of(W * j, W)
    yield 2, (pl.ds(at, W), pl.ds(0, C)), (pl.ds(2 * RD, W), pl.ds(0, C))
    yield 2, (pl.ds(at, W // 2), pl.ds(C, D - C)), (pl.ds(2 * RD + W, W // 2), pl.ds(0, D - C))
    yield 2, (pl.ds(at + W // 2, W // 2), pl.ds(C, D - C)), (pl.ds(2 * RD + W, W // 2), pl.ds(D - C, D - C))


def place():
    me, y = lax.axis_index("s"), lax.axis_index("r")
    return me, y, {"s": me + 1 - 2 * lax.rem(me, 2)}, {"s": lax.rem(me + 2, S)}, {"r": 1 - y}


def greet():
    _, _, core, across, copy = place()
    barrier = pltpu.get_barrier_semaphore()
    for to in (core, across, copy):
        pl.semaphore_signal(barrier, inc=1, device_id=to, device_id_type=MESH)
    pl.semaphore_wait(barrier, 3)


def remote(src, dst, send, recv, to):
    return pltpu.make_async_remote_copy(src_ref=src, dst_ref=dst, send_sem=send, recv_sem=recv, device_id=to, device_id_type=MESH)


FROM = (0, 1, 2, 0, 0)


def wait_pieces(whole, n, sem):
    ref = whole.at[0, pl.ds(0, n), 0]
    pltpu.make_async_copy(ref, ref, sem).wait()


class Gather:
    def __init__(self, first, mine, whole, stage, send, recv, local):
        self.first, self.mine, self.whole, self.stage = first, mine, whole, stage
        self.send, self.recv, self.local, self.ring = send, recv, local, stage.shape[0]

    @staticmethod
    def scratch(n, ring):
        return [
            pltpu.VMEM((ring, PR, C), bf16),
            pltpu.SemaphoreType.DMA((ring,)),
            pltpu.SemaphoreType.DMA((n, 3)),
            pltpu.SemaphoreType.DMA((ring, 2)),
        ]

    def copy(self, k, n):
        me, y, core, across, copy = place()
        l, j, slot = k // J, lax.rem(k, J), lax.rem(k, self.ring)
        near, far = pl.ds(pl.multiple_of(HALF * y, HALF), HALF), pl.ds(pl.multiple_of(HALF * (1 - y), HALF), HALF)
        rows = ((), (near,), (near,), (near,), (far,))[n]
        s = me if n < 2 else lax.rem(me + 2, S)
        what = self.whole.at[(l, s, j, *rows)]
        src = self.stage.at[(slot, *rows)] if n < 2 else what
        return remote(src, what, self.send.at[slot], self.recv.at[k - self.first, FROM[n]], (core, across, copy, core, core)[n])

    def keep(self, k):
        slot = lax.rem(k, self.ring)
        return pltpu.make_async_copy(self.stage.at[slot], self.whole.at[k // J, place()[0], lax.rem(k, J)], self.local.at[slot, 1])

    def pack(self, k):
        slot = lax.rem(k, self.ring)
        for m, src, dst in piece_slices(lax.rem(k, J)):
            pltpu.make_async_copy(self.mine[m].at[(k // J, *src)], self.stage.at[(slot, *dst)], self.local.at[slot, 0]).start()

    def start(self, k):
        slot = lax.rem(k, self.ring)
        pltpu.make_async_copy(self.stage.at[slot], self.stage.at[slot], self.local.at[slot, 0]).wait()
        self.copy(k, 1).start()
        self.copy(k, 0).start()
        self.keep(k).start()

    def across(self, k):
        self.copy(k, 1).wait_recv()
        self.copy(k, 2).start()
        self.copy(k, 3).start()

    def along(self, k):
        self.copy(k, 2).wait_recv()
        self.copy(k, 4).start()

    def finish(self, k):
        wait_pieces(self.whole, 2, self.recv.at[k - self.first, 0])
        wait_pieces(self.whole, 3, self.send.at[lax.rem(k, self.ring)])
        self.keep(k).wait()


def fetch(whole, held, sem, l, j):
    slot = lax.rem(j, 2)
    return pltpu.make_async_copy(whole.at[l, :, j], held.at[slot], sem.at[slot])


SWIFT = 2
PARTS = 3
ALL, SOON, LATE = (0, PARTS), (0, PARTS - 1), (PARTS - 1, PARTS)


class Swift(Gather):
    def __init__(self, mine, whole, held, send, recv, local):
        self.mine, self.whole, self.held, self.send, self.recv, self.local = mine, whole, held, send, recv, local

    SCRATCH = [pltpu.SemaphoreType.DMA((SWIFT,)), pltpu.SemaphoreType.DMA((SWIFT, 3, PARTS)), pltpu.SemaphoreType.DMA((SWIFT, 2))]

    def copies(self, k, n, parts=ALL):
        me, y, core, across, copy = place()
        s = me if n < 2 else lax.rem(me + 2, S)
        to = (core, across, copy, core, core)[n]
        for i in range(*parts) if n else (0,):
            rows = HALF * (1 - y if n == 4 else y) + HALF // PARTS * i
            what = self.held.at[(k, s, pl.ds(pl.multiple_of(rows, HALF // PARTS), HALF // PARTS)) if n else (k, s)]
            yield remote(what, what, self.send.at[k], self.recv.at[k, FROM[n], i if FROM[n] else 0], to)

    def keep(self, k):
        return pltpu.make_async_copy(self.held.at[k], self.whole.at[0, :, k], self.local.at[k, 1])

    def pack(self, k):
        for m, src, dst in piece_slices(k):
            pltpu.make_async_copy(self.mine[m].at[(0, *src)], self.held.at[(k, place()[0], *dst)], self.local.at[k, 0]).start()

    def start(self, k):
        own = self.held.at[k, place()[0]]
        pltpu.make_async_copy(own, own, self.local.at[k, 0]).wait()
        for n in (1, 0):
            for copy in self.copies(k, n):
                copy.start()

    def across(self, k, parts=ALL):
        for x, y, core in zip(*(self.copies(k, n, parts) for n in (1, 2, 3))):
            x.wait_recv()
            y.start()
            core.start()

    def along(self, k, parts=ALL):
        for y, core in zip(*(self.copies(k, n, parts) for n in (2, 4))):
            y.wait_recv()
            core.start()

    def finish(self, k):
        wait_pieces(self.whole, 2, self.recv.at[k, 0, 0])
        wait_pieces(self.whole, 3, self.send.at[k])
        self.keep(k).start()


def rows_of(t, T):
    return pl.ds(pl.multiple_of(t * T, T), T)


def in_turn(low, high, f):
    def body(i, _):
        f(i)
        return 0

    lax.fori_loop(low, high, body, 0)


def by_rows(low, high, f):
    n = 256
    in_turn(low // n, high // n, lambda i: f(rows_of(i, n)))


def forward_kernel(T, x_i, wg, wu, wd, h_o, a0_o, a1_o, saved, whole, x, a, acc, held, load, io, first, *rest):
    j, t = place_in_grid()
    swift = Swift((wg, wu, wd), whole, held, *rest[:3])
    gather = Gather(SWIFT, (wg, wu, wd), whole, *rest[3:])
    ahead, K, NT = 4, J + EARLY, TOK // T
    assert NT == 2 and SWIFT == 2 and EARLY == 2
    rows = pl.ds(pl.multiple_of(t * T, T), T)

    def outs(t):
        part = pl.ds(pl.multiple_of(t * T, T), T)
        return [pltpu.make_async_copy(x.at[part], h_o.at[part], io.at[1, t]), pltpu.make_async_copy(a.at[part], a1_o.at[part], io.at[2, t])]

    def take(j):
        fetch(whole, held, load, 0, j).start()

    @pl.when((j == 0) & (t == 0))
    def _():
        n = 4
        states = lambda i: pltpu.make_async_copy(x_i.at[rows_of(i, TOK // n)], x.at[rows_of(i, TOK // n)], first.at[i])
        swift.pack(0)
        states(0).start()
        swift.pack(1)
        for i in range(1, n):
            states(i).start()
        greet()
        for k in range(SWIFT):
            swift.start(k)
        in_turn(SWIFT, ahead + 2, gather.pack)

        def norm(i):
            states(i).wait()

            def some(rows):
                a[rows, :] = normed(x[rows, :].astype(f32))

            by_rows(TOK // n * i, TOK // n * (i + 1), some)

        norm(0)
        swift.across(0)
        gather.start(SWIFT)
        in_turn(1, n, norm)
        pltpu.make_async_copy(a, a0_o, io.at[0, 1]).start()
        swift.along(0)
        in_turn(SWIFT + 1, ahead + 1, gather.start)
        swift.across(1, SOON)
        swift.finish(0)

    @pl.when((t == 0) & (j > 0))
    def _():
        @pl.when(j == 1)
        def _():
            swift.along(1, LATE)
            swift.finish(1)

        @pl.when(j >= SWIFT)
        def _():
            fetch(whole, held, load, 0, j).wait()

            gather.along(j + 1)

        @pl.when(j < LAST)
        def _():
            gather.across(j + 2)

        @pl.when(j == LAST)
        def _():
            gather.along(J + 1)

        @pl.when(j + ahead < K)
        def _():
            gather.start(j + ahead)

        @pl.when(j + ahead + 1 < K)
        def _():
            gather.pack(j + ahead + 1)

    @pl.when(t == 1)
    def _():
        @pl.when(j == 0)
        def _():
            swift.across(1, LATE)
            swift.along(1, SOON)
            gather.across(SWIFT)

        @pl.when(j == 1)
        def _():
            gather.along(2)

        @pl.when(j > 0)
        def _():
            gather.finish(j + 1)

        @pl.when((j == 1) | (j == 2))
        def _():
            swift.keep(j - 1).wait()

        @pl.when((j > 0) & (j + 1 < J))
        def _():
            take(j + 1)

        @pl.when(j == J - 2)
        def _():
            gather.across(J + 1)

        @pl.when(j == LAST)
        def _():
            gather.finish(J + 1)

    w = held.at[lax.rem(j, 2)]
    n = T // BLOCKS
    for i in range(BLOCKS):
        part, rows = slice(i * n, (i + 1) * n), rows_of(BLOCKS * t + i, n)
        lhs = a[rows, :]
        g, u = dot(lhs, gate_of(w)), dot(lhs, up_of(w))
        saved[0, 0, part], saved[0, 1, part] = g, u
        act = (g * jax.nn.sigmoid(g) * u).astype(bf16)
        acc[rows, :] = jnp.where(j == 0, 0.0, acc[rows, :]) + dot(act, down_of(w))

    @pl.when(j == LAST)
    def _():
        @pl.when(t == 0)
        def _():
            pltpu.make_async_copy(a, a0_o, io.at[0, 1]).wait()

        def some(rows):
            h = (x[rows, :].astype(f32) + acc[rows, :].astype(bf16).astype(f32)).astype(bf16)
            x[rows, :] = h
            a[rows, :] = normed(h.astype(f32))

        by_rows(t * T, (t + 1) * T, some)
        for copy in outs(t):
            copy.start()

        @pl.when(t == NT - 1)
        def _():
            for i in range(NT):
                for copy in outs(i):
                    copy.wait()


def forward(x, wg, wu, wd):
    T = 2048
    tile = pl.BlockSpec((1, 2, T, C), lambda j, t: (j, 0, t, 0))
    states = jax.ShapeDtypeStruct((TOK, D), bf16)
    return pl.pallas_call(
        functools.partial(forward_kernel, T),
        grid=(J, TOK // T),
        in_specs=[hbm] * 4,
        out_specs=[hbm] * 3 + [tile, hbm],
        out_shape=[states] * 3 + [jax.ShapeDtypeStruct((J, 2, TOK, C), f32)] + [jax.ShapeDtypeStruct((L, S, J, PR, C), bf16)],
        scratch_shapes=[
            pltpu.VMEM((TOK, D), bf16),
            pltpu.VMEM((TOK, D), bf16),
            pltpu.VMEM((TOK, D), f32),
            pltpu.VMEM((2, S, PR, C), bf16),
            pltpu.SemaphoreType.DMA((2,)),
            pltpu.SemaphoreType.DMA((3, 2)),
            pltpu.SemaphoreType.DMA((4,)),
        ]
        + Swift.SCRATCH
        + Gather.scratch(J + EARLY - SWIFT, 6),
        **params(3, 250, collective_id=0, has_side_effects=True),
        name="forward",
    )(x, wg, wu, wd)


def pack(s, ag, au, ad):
    rows, down = pl.ds(pl.multiple_of(RD * s, RD), RD), pl.multiple_of(W * s, W)
    yield slice(0, RD), slice(0, C), ag[rows, :]
    yield slice(RD, 2 * RD), slice(0, C), au[rows, :]
    yield slice(2 * RD, 2 * RD + W), slice(0, C), ad[pl.ds(down, W), :C]
    yield slice(2 * RD + W, PR), slice(0, D - C), ad[pl.ds(down, W // 2), C:]
    yield slice(2 * RD + W, PR), slice(D - C, C), ad[pl.ds(down + W // 2, W // 2), C:]


class Reduce:
    def __init__(self, sums, theirs, kept, out_a, in_a, kept_b, out_b, in_b, out_c, sems):
        self.sums, self.theirs = sums, theirs
        self.kept, self.out_a, self.in_a = kept, out_a, in_a
        self.kept_b, self.out_b, self.in_b, self.out_c = kept_b, out_b, in_b, out_c
        self.sems = sems

    SCRATCH = [
        pltpu.VMEM((2, PR, C), f32),
        pltpu.VMEM((2, PR, C), bf16),
        pltpu.VMEM((2, 2, PR, C), bf16),
        pltpu.VMEM((PR, C), f32),
        pltpu.VMEM((PR, C), bf16),
        pltpu.VMEM((2, PR, C), bf16),
        pltpu.VMEM((PR, C), bf16),
        pltpu.SemaphoreType.DMA((3, 4)),
    ]

    def at(self, sums, theirs):
        return Reduce(sums, theirs, self.kept, self.out_a, self.in_a, self.kept_b, self.out_b, self.in_b, self.out_c, self.sems)

    def copy_a(self, j, src=None):
        slot = lax.rem(j, 2)
        return remote(self.out_a if src is None else src, self.in_a.at[slot], self.sems.at[0, 0], self.sems.at[0, 1 + slot], place()[2])

    def copy_b(self, j):
        slot = lax.rem(j, 2)
        return remote(self.out_b, self.in_b.at[slot], self.sems.at[1, 0], self.sems.at[1, 1 + slot], place()[3])

    def copy_c(self, j):
        return remote(self.out_c, self.theirs.at[j], self.sems.at[2, 0], self.sems.at[2, 1 + lax.rem(j, 2)], place()[4])

    def store_c(self, j):
        return pltpu.make_async_copy(self.out_c, self.sums.at[j], self.sems.at[2, 3])

    def again_c(self, j, send, recv):
        return remote(self.sums.at[j], self.theirs.at[j], send, recv, place()[4])

    def collect(self, ag, au, ad):
        c = lax.rem(lax.axis_index("s"), 2)
        for x in range(2):
            for r, cols, v in pack(2 * x + 1 - c, ag, au, ad):
                self.out_a[x, r, cols] = v.astype(bf16)
            for r, cols, v in pack(2 * x + c, ag, au, ad):
                self.kept[x, r, cols] = v

    def step_a(self, j):
        self.copy_a(j).wait()
        slot, x = lax.rem(j, 2), lax.axis_index("s") // 2
        self.out_b[...] = (self.kept[1 - x] + self.in_a[slot, 1 - x].astype(f32)).astype(bf16)
        self.copy_b(j).start()
        self.kept_b[...] = self.kept[x] + self.in_a[slot, x].astype(f32)

    def step_b(self, j, send=True):
        self.copy_b(j).wait()
        self.out_c[...] = (self.kept_b[...] + self.in_b[lax.rem(j, 2)].astype(f32)).astype(bf16)
        if send:
            self.copy_c(j).start()
        self.store_c(j).start()

    def step_c(self, j):
        self.copy_c(j).wait()
        self.store_c(j).wait()

    def follow(self, j):
        for stage, step in ((3, self.step_c), (2, self.step_b), (1, self.step_a)):
            pl.when(j >= stage)(functools.partial(step, j - stage))

    def handed(self, kept, out_a, sems):
        return [pltpu.make_async_copy(src, dst, sems.at[i]) for i, (src, dst) in enumerate(((self.kept, kept), (self.out_a, out_a)))]

    def leave(self, copies):
        self.step_c(J - 3)
        self.step_b(J - 2, send=False)
        self.store_c(J - 2).wait()
        for copy in copies:
            copy.wait()


def gradients(by, g, u):
    sig = jax.nn.sigmoid(g)
    silu = g * sig
    return (silu * u).astype(bf16), (by * u * (sig + silu * (1 - sig))).astype(bf16), (by * silu).astype(bf16)


def accumulate(t, a, dy, act, dg, du, ag, au, ad):
    both = dot(a, jnp.concatenate([dg, du], axis=1), 0, 0)
    for acc, term in ((ag, both[:, :C]), (au, both[:, C:]), (ad, dot(act, dy, 0, 0))):
        acc[...] = jnp.where(t == 0, 0.0, acc[...]) + term


PIECE = 512


class Pair:
    def __init__(self, *copies):
        self.copies = copies

    def start(self):
        for copy in self.copies:
            copy.start()

    def wait(self):
        for copy in self.copies:
            copy.wait()


def state_copies(i, first, second, sems):
    rows = rows_of(i, PIECE)
    return Pair(*(pltpu.make_async_copy(src.at[rows], dst.at[rows], sems.at[n, i]) for n, (src, dst) in enumerate((first, second))))


def second_kernel(a_i, dy_i, h, wg, wu, wd, _, out, sums, theirs, kept_o, out_o, whole, a, dy, ag, au, ad, total, held, load, save, states, *rest):
    j, t = place_in_grid()
    NT = 4
    T = TOK // NT
    gather = Gather(J + EARLY, (wg, wu, wd), whole, *rest[:4])
    reduce = Reduce(sums, theirs, *rest[4:])
    lead = EARLY + 1
    rows = rows_of(t, T)

    parts = T // PIECE

    def inputs(i):
        return state_copies(i, (a_i, a), (dy_i, dy), states)

    def layer_input(i):
        return pltpu.make_async_copy(h.at[rows_of(i, PIECE)], a.at[rows_of(i, PIECE)], states.at[0, i])

    def result(i):
        return pltpu.make_async_copy(dy.at[rows_of(i, PIECE)], out.at[rows_of(i, PIECE)], states.at[1, i])

    @pl.when((j == 0) & (t == 0))
    def _():
        in_turn(J + EARLY, J + lead + 1, gather.pack)
        fetch(whole, held, load, 1, 0).start()
        in_turn(0, NT * parts, lambda i: inputs(i).start())
        greet()
        gather.start(J + EARLY)

    @pl.when(j == 0)
    def _():
        in_turn(parts * t, parts * (t + 1), lambda i: inputs(i).wait())

    @pl.when(t == 0)
    def _():
        fetch(whole, held, load, 1, j).wait()

        @pl.when((j + 1 >= EARLY) & (j + 1 < J))
        def _():
            gather.along(J + j + 1)

        @pl.when(j + lead < J)
        def _():
            gather.start(J + j + lead)

        @pl.when(j + lead + 1 < J)
        def _():
            gather.pack(J + j + lead + 1)

    @pl.when(t == 1)
    def _():
        reduce.follow(j)

    @pl.when((t == 2) & (j + 2 < J))
    def _():
        gather.across(J + j + 2)

    @pl.when((t == 3) & (j + 1 < J))
    def _():
        @pl.when(j + 1 >= EARLY)
        def _():
            gather.finish(J + j + 1)

        fetch(whole, held, load, 1, j + 1).start()

    w = held.at[lax.rem(j, 2)]
    lhs, ct = a[rows, :], dy[rows, :]
    gate, up = gate_of(w), up_of(w)
    g, u = dot(lhs, gate), dot(lhs, up)
    by = dot_across(ct, down_of(w)).astype(bf16).astype(f32)
    act, dg, du = gradients(by, g, u)
    accumulate(t, lhs, ct, act, dg, du, ag, au, ad)
    total[rows, :] = jnp.where(j == 0, 0.0, total[rows, :]) + (dot_across(dg, gate) + dot_across(du, up))

    @pl.when(t == NT - 1)
    def _():
        reduce.collect(ag, au, ad)

        @pl.when(j < LAST)
        def _():
            reduce.copy_a(j).start()

    @pl.when(j == LAST)
    def _():
        in_turn(parts * t, parts * (t + 1), lambda i: layer_input(i).start())

        @pl.when(t == NT - 1)
        def _():
            copies = reduce.handed(kept_o, out_o, save)
            for copy in copies:
                copy.start()

            def back(i):
                layer_input(i).wait()

                def some(rows):
                    dy[rows, :] = norm_back(total[rows, :], a[rows, :], dy[rows, :])

                by_rows(i * PIECE, (i + 1) * PIECE, some)
                result(i).start()

            in_turn(0, NT * parts, back)
            reduce.leave(copies)
            in_turn(0, NT * parts, lambda i: result(i).wait())


PIECES = jax.ShapeDtypeStruct((J, PR, C), bf16)


def second_pass(a, dy, h, wg, wu, wd, whole):
    T = TOK // 4
    return pl.pallas_call(
        second_kernel,
        grid=(J, TOK // T),
        in_specs=[hbm] * 7,
        out_specs=[hbm] * 6,
        out_shape=[jax.ShapeDtypeStruct((TOK, D), bf16), PIECES, PIECES]
        + [jax.ShapeDtypeStruct((2, PR, C), f32), jax.ShapeDtypeStruct((2, PR, C), bf16), jax.ShapeDtypeStruct((L, S, J, PR, C), bf16)],
        scratch_shapes=[
            pltpu.VMEM((TOK, D), bf16),
            pltpu.VMEM((TOK, D), bf16),
            pltpu.VMEM((D, C), f32),
            pltpu.VMEM((D, C), f32),
            pltpu.VMEM((C, D), f32),
            pltpu.VMEM((TOK, D), f32),
            pltpu.VMEM((2, S, PR, C), bf16),
            pltpu.SemaphoreType.DMA((2,)),
            pltpu.SemaphoreType.DMA((2,)),
            pltpu.SemaphoreType.DMA((2, TOK // PIECE)),
        ]
        + Gather.scratch(J - EARLY, 4)
        + Reduce.SCRATCH,
        input_output_aliases={6: 5},
        **params(8, 100, collective_id=1, has_side_effects=True),
        name="second_pass",
    )(a, dy, h, wg, wu, wd, whole)


def first_kernel(a_i, dy_i, w, gu, s1_i, t1_i, kept_i, out_i, cts, sums, theirs, kept_o, out_o, s1, t1, a, dy, ag, au, ad, save, states, *rest):
    j, t = place_in_grid()
    T = cts.shape[2]
    NT = TOK // T
    rows = rows_of(t, T)
    reduce = Reduce(sums, theirs, *rest)
    before = reduce.at(s1, t1)
    kept = lambda: pltpu.make_async_copy(kept_i, reduce.kept, save.at[0])
    again = lambda: before.again_c(J - 2, save.at[1], save.at[2])

    parts = T // PIECE

    def inputs(i):
        return state_copies(i, (a_i, a), (dy_i, dy), states)

    @pl.when((j == 0) & (t == 0))
    def _():
        in_turn(0, parts, lambda i: inputs(i).start())
        kept().start()
        in_turn(parts, NT * parts, lambda i: inputs(i).start())
        greet()
        before.copy_a(LAST, out_i).start()
        again().start()

    @pl.when(j == 0)
    def _():
        in_turn(parts * t, parts * (t + 1), lambda i: inputs(i).wait())

    @pl.when(t == 1)
    def _():
        @pl.when(j == 2)
        def _():
            before.step_c(LAST)

        @pl.when(j == 1)
        def _():
            again().wait()
            before.step_b(LAST)

        @pl.when(j == 0)
        def _():
            kept().wait()
            before.step_a(LAST)

        reduce.follow(j)

    lhs, ct = a[rows, :], dy[rows, :]
    by = dot_across(ct, down_of(w.at[0, :, 0], 0)).astype(bf16).astype(f32)
    act, dg, du = gradients(by, gu[0, 0], gu[0, 1])
    cts[0, 0], cts[0, 1] = dg, du
    accumulate(t, lhs, ct, act, dg, du, ag, au, ad)

    @pl.when(t == NT - 1)
    def _():
        reduce.collect(ag, au, ad)

        @pl.when(j < LAST)
        def _():
            reduce.copy_a(j).start()

        @pl.when(j == LAST)
        def _():
            copies = reduce.handed(kept_o, out_o, save)
            for copy in copies:
                copy.start()
            reduce.leave(copies)


def first_pass(a, dy, whole, gu, s1, t1, kept, out_a):
    T = 1024
    tile = pl.BlockSpec((1, 2, T, C), lambda j, t: (j, 0, t, 0))
    return pl.pallas_call(
        first_kernel,
        grid=(J, TOK // T),
        in_specs=[hbm, hbm, pl.BlockSpec((1, S, 1, PR - 2 * RD, C), lambda j, t: (0, 0, j, 2, 0)), tile] + [hbm] * 4,
        out_specs=[tile] + [hbm] * 6,
        out_shape=[jax.ShapeDtypeStruct((J, 2, TOK, C), bf16)]
        + [PIECES, PIECES, jax.ShapeDtypeStruct((2, PR, C), f32), jax.ShapeDtypeStruct((2, PR, C), bf16), PIECES, PIECES],
        scratch_shapes=[
            pltpu.VMEM((TOK, D), bf16),
            pltpu.VMEM((TOK, D), bf16),
            pltpu.VMEM((D, C), f32),
            pltpu.VMEM((D, C), f32),
            pltpu.VMEM((C, D), f32),
            pltpu.SemaphoreType.DMA((3,)),
            pltpu.SemaphoreType.DMA((2, TOK // PIECE)),
        ]
        + Reduce.SCRATCH,
        input_output_aliases={4: 5, 5: 6},
        **params(4, 300, collective_id=2, has_side_effects=True),
        name="first_pass",
    )(a, dy, whole, gu, s1, t1, kept, out_a)


PART = TOK // 2


Q = 2
STEPS = J // Q
END = STEPS - 1


def contract(j, cts, w, acc):
    n = PART // Q
    for i in range(PART // n):
        rows = slice(i * n, (i + 1) * n)
        total = jnp.where(j == 0, 0.0, acc[rows, :])
        for q in range(Q):
            held = w.at[0, :, q]
            total = total + (dot_across(cts[q, 0, rows], gate_of(held)) + dot_across(cts[q, 1, rows], up_of(held)))
        acc[rows, :] = total


def input_kernel(cts, w, h_i, dy_i, s1, t1, s_i, t_i, kept_i, out_i, g1, out, sums, theirs, acc, h, dy, save, states, *rest):
    reduce = Reduce(sums, theirs, *rest)
    j = pl.program_id(0)
    late_states(0, j, h_i, dy_i, h, dy, states)

    @pl.when(j == 0)
    def _():
        pltpu.make_async_copy(kept_i, reduce.kept, save.at[0]).start()
        greet()
        reduce.copy_a(LAST, out_i).start()
        reduce.again_c(J - 2, save.at[1], save.at[2]).start()

    @pl.when(j == 1)
    def _():
        pltpu.make_async_copy(kept_i, reduce.kept, save.at[0]).wait()
        reduce.step_a(LAST)

    @pl.when(j == 3)
    def _():
        reduce.step_b(LAST)

    @pl.when(j == END)
    def _():
        reduce.again_c(J - 2, save.at[1], save.at[2]).wait()
        reduce.step_c(LAST)

    g1[...] = (s1[...].astype(f32) + t1[...].astype(f32)).astype(bf16)
    contract(j, cts, w, acc)

    @pl.when(j == END)
    def _():
        def some(rows):
            out[rows, :] = norm_back(acc[rows, :], h[rows, :], dy[rows, :])

        by_rows(0, PART, some)


def late_states(part, j, h_i, dy_i, h, dy, sems):
    copies = lambda: [pltpu.make_async_copy(src.at[pl.ds(part * PART, PART)], dst, sems.at[i]) for i, (src, dst) in enumerate(((h_i, h), (dy_i, dy)))]

    @pl.when(j == 2)
    def _():
        for copy in copies():
            copy.start()

    @pl.when(j == END)
    def _():
        for copy in copies():
            copy.wait()


STATES = [pltpu.VMEM((PART, D), f32), pltpu.VMEM((PART, D), bf16), pltpu.VMEM((PART, D), bf16)]
piece = pl.BlockSpec((Q, PR, C), lambda j: (j, 0, 0))


def part_specs(part):
    return [pl.BlockSpec((Q, 2, PART, C), lambda j: (j, 0, part, 0)), pl.BlockSpec((1, S, Q, 2 * RD, C), lambda j: (0, 0, j, 0, 0)), hbm, hbm]


def input_pass(cts, whole, h, dy, s1, t1, sums, theirs, kept, out_a):
    return pl.pallas_call(
        input_kernel,
        grid=(STEPS,),
        in_specs=part_specs(0) + [piece, piece] + [hbm] * 4,
        out_specs=[piece, pl.BlockSpec((PART, D), lambda j: (0, 0), pipeline_mode=once), hbm, hbm],
        out_shape=[PIECES, jax.ShapeDtypeStruct((PART, D), bf16), PIECES, PIECES],
        scratch_shapes=STATES + [pltpu.SemaphoreType.DMA((3,)), pltpu.SemaphoreType.DMA((2,))] + Reduce.SCRATCH,
        input_output_aliases={6: 2, 7: 3},
        **params(1, 100, collective_id=3, has_side_effects=True),
        name="input_pass",
    )(cts, whole, h, dy, s1, t1, sums, theirs, kept, out_a)


def last_kernel(cts, w, h_i, dy_i, g1, s0, t0, begun, out, og, ou, od, acc, h, dy, stage, passing, sems, io, states):
    j = pl.program_id(0)
    late_states(1, j, h_i, dy_i, h, dy, states)
    slot = lax.rem(j, 2)
    first = lambda: pltpu.make_async_copy(begun, passing, io.at[0])
    second = lambda: pltpu.make_async_copy(passing, out.at[0], io.at[1])

    def wait(slot):
        for l in range(L):
            pltpu.make_async_copy(stage.at[slot, l], stage.at[slot, l], sems.at[slot, l]).wait()

    @pl.when(j == 0)
    def _():
        first().start()

    @pl.when(j == 2)
    def _():
        first().wait()
        second().start()

    @pl.when(j >= 2)
    def _():
        wait(slot)

    stage[slot, 0] = (s0[...].astype(f32) + t0[...].astype(f32)).astype(bf16)
    stage[slot, 1] = g1[...]
    contract(j, cts, w, acc)
    for l in range(L):

        def unpack(q):
            for m, dst, src in piece_slices(Q * j + q):
                pltpu.make_async_copy(stage.at[(slot, l, q, *src)], (og, ou, od)[m].at[(l, *dst)], sems.at[slot, l]).start()

        in_turn(0, Q, unpack)

    @pl.when(j == END)
    def _():
        n = 4
        result = lambda i: pltpu.make_async_copy(dy.at[rows_of(i, PART // n)], out.at[1, rows_of(i, PART // n)], io.at[2 + i])

        def quarter(i):
            def some(rows):
                dy[rows, :] = norm_back(acc[rows, :], h[rows, :], dy[rows, :])

            by_rows(PART // n * i, PART // n * (i + 1), some)
            result(i).start()

        in_turn(0, n, quarter)
        wait(1 - slot)
        wait(slot)
        second().wait()
        in_turn(0, n, lambda i: result(i).wait())


def last_pass(cts, whole, h, dy, g1, s0, t0, begun):
    return pl.pallas_call(
        last_kernel,
        grid=(STEPS,),
        in_specs=part_specs(1) + [piece] * 3 + [hbm],
        out_specs=[hbm] * 4,
        out_shape=[jax.ShapeDtypeStruct((2, PART, D), bf16)] + [jax.ShapeDtypeStruct((L, RD, FF), bf16)] * 2 + [jax.ShapeDtypeStruct((L, RF, D), bf16)],
        scratch_shapes=STATES
        + [
            pltpu.VMEM((2, L, Q, PR, C), bf16),
            pltpu.VMEM((PART, D), bf16),
            pltpu.SemaphoreType.DMA((2, L)),
            pltpu.SemaphoreType.DMA((6,)),
            pltpu.SemaphoreType.DMA((2,)),
        ],
        **params(1, 150),
        name="last_pass",
    )(cts, whole, h, dy, g1, s0, t0, begun)


def solution(mesh):
    def step(x, dy, *weights):
        x, dy = x[0], dy[0]
        h1, a0, a1, gu, whole = forward(x, *weights)
        by1, s1, t1, kept, out_a, whole = second_pass(a1, dy, h1, *weights, whole)
        cts, s0, t0, kept, out_a, s1, t1 = first_pass(a0, by1, whole, gu, s1, t1, kept, out_a)
        g1, begun, s0, t0 = input_pass(cts, whole, x, by1, s1, t1, s0, t0, kept, out_a)
        by0, *grads = last_pass(cts, whole, x, by1, g1, s0, t0, begun)
        return (by0.reshape(1, TOK, D), *grads)

    states, cut = P(("rep", "r", "s"), None, None), P(None, "s", None)
    return jax.shard_map(
        step,
        mesh=mesh,
        in_specs=(states, states) + (cut,) * 3,
        out_specs=(states,) + (P("rep", "s", None),) * 3,
        check_vma=False,
    )
```
